256 devices in a mesh: img: 16 (over y, x), row: 16 (over z, core).
Axes of the slice: x: 4, y: 4, z: 8, core: 2. Of those that a mesh axis runs over, the one named last changes fastest.
Arguments:
- latent: bfloat16 [1024, 128, 512], P(('img', 'row')), parts along dimension 0, may hold values from -8 to 8
- attn_gain: float32 [512], replicated, may hold values from 0.5 to 1.5
- attn_shift: float32 [512], replicated, may hold values from -3 to 3
- w_query: bfloat16 [512, 512], replicated, may hold values from -2 to 2
- w_key: bfloat16 [512, 512], replicated, may hold values from -2 to 2
- w_value: bfloat16 [512, 512], replicated, may hold values from -0.25 to 0.25
- w_out: bfloat16 [512, 512], replicated, may hold values from -0.25 to 0.25
- conv_gain: float32 [512], replicated, may hold values from 0.5 to 1.5
- conv_shift: float32 [512], replicated, may hold values from -3 to 3
- w_conv: bfloat16 [3, 3, 512, 512], replicated, may hold values from -0.09375 to 0.09375
- conv_bias: float32 [512], replicated, may hold values from -3 to 3
Outputs:
- encoded: bfloat16 [1024, 128, 512], P(('img', 'row')), parts along dimension 0
The draws below stay inside these ranges and needn't reach their ends.
There are 16 independent parts, one for each index of `img`. The reference program is written for one: setup_inputs(seed, part) draws one part's arguments, and reference() takes and returns one part's arrays. A program takes and returns all parts, laid end to end along the dimension named above; an argument that names none is the same for every part. Nothing has to cross between parts.
All inputs are finite; a program needn't handle non-finite values.
Results may differ from the reference program's by a relative error of at most 0.011.
Values may be sent and summed in bfloat16 or wider, within the bound.
A program may use at most 128 MiB of HBM per device.

```python
import jax
import jax.numpy as jnp
from jax import lax

C = 512
GROUPS = 32
W = 128
H = 64


def shared_gauss(key):
    return jnp.clip(jax.random.normal(jax.random.fold_in(key, 7), (C, C), jnp.float32), -3.0, 3.0)


def draw_latent(key, part):
    noise = jax.random.normal(jax.random.fold_in(key, 3), (H, W, C), jnp.float32)
    rows = (jnp.arange(H, dtype=jnp.float32) + 0.5) / H
    phase = jax.random.uniform(jax.random.fold_in(key, 13), (GROUPS,), jnp.float32, -jnp.pi, jnp.pi)
    amplitude = jax.random.uniform(jax.random.fold_in(key, 17), (C,), jnp.float32, 0.8, 1.6)
    wave = jnp.sin(2.0 * jnp.pi * rows[:, None] + phase[None, :])
    offset = jnp.repeat(wave, C // GROUPS, axis=1) * amplitude[None, :]
    result = noise + offset[:, None, :]
    return jnp.clip(result, -8.0, 8.0).astype(jnp.bfloat16)


def draw_w_query(key, part):
    return (shared_gauss(key) * (4.0 / jnp.sqrt(jnp.float32(C)))).astype(jnp.bfloat16)


def draw_w_key(key, part):
    fresh = jnp.clip(jax.random.normal(jax.random.fold_in(key, 11), (C, C), jnp.float32), -3.0, 3.0)
    result = fresh / jnp.sqrt(jnp.float32(C))
    return result.astype(jnp.bfloat16)


def scatter_about(stream_key, extent, scale, most, kind=jnp.bfloat16):
    return jnp.clip(scale * jax.random.normal(stream_key, extent, jnp.float32), -most, most).astype(kind)


def setup_inputs(seed: int = 0, part: int = 0) -> dict:
    key_list = jax.random.split(jax.random.key(seed), 12)
    part_splits = jax.random.split(jax.random.fold_in(key_list[11], part), 12)
    return {
        "latent": draw_latent(jax.random.fold_in(jax.random.fold_in(key_list[11], part), 71), part),
        "attn_gain": jnp.clip(1.0 + 0.1 * jax.random.normal(key_list[1], (C,), jnp.float32), 0.5, 1.5),
        "attn_shift": scatter_about(key_list[2], (C,), 0.5, 3.0, jnp.float32),
        "w_query": draw_w_query(jax.random.fold_in(key_list[11], 71), part),
        "w_key": draw_w_key(jax.random.fold_in(key_list[11], 71), part),
        "w_value": scatter_about(key_list[5], (C, C), C ** -0.5, 0.25),
        "w_out": scatter_about(key_list[6], (C, C), C ** -0.5, 0.25),
        "conv_gain": jnp.clip(1.0 + 0.1 * jax.random.normal(key_list[7], (C,), jnp.float32), 0.5, 1.5),
        "conv_shift": scatter_about(key_list[8], (C,), 0.5, 3.0, jnp.float32),
        "w_conv": scatter_about(key_list[9], (3, 3, C, C), (9 * C) ** -0.5, 0.09375),
        "conv_bias": scatter_about(key_list[10], (C,), 0.5, 3.0, jnp.float32),
    }


epsilon = 1e-06

def group_norm(field, gain, shift):
    grouped = field.astype(jnp.float32).reshape(field.shape[0], GROUPS, C // GROUPS)
    centre = lax.optimization_barrier(jnp.mean(grouped, axis=(0, 2)))
    offset = grouped - centre[None, :, None]
    spread = lax.optimization_barrier(jnp.mean(offset * offset, axis=(0, 2)))
    normed = offset * lax.rsqrt(spread + epsilon)[None, :, None]
    return normed.reshape(field.shape) * gain + shift

def reference(latent, attn_gain, attn_shift, w_query, w_key, w_value, w_out, conv_gain, conv_shift, w_conv, conv_bias):
    positions = latent.reshape(H * W, C)
    normed = group_norm(positions, attn_gain, attn_shift).astype(jnp.bfloat16)
    queries = jnp.dot(normed, w_query, preferred_element_type=jnp.float32).astype(jnp.bfloat16)
    key_rows = jnp.dot(normed, w_key, preferred_element_type=jnp.float32).astype(jnp.bfloat16)
    values = jnp.dot(normed, w_value, preferred_element_type=jnp.float32).astype(jnp.bfloat16)
    scaling = 1.0 / jnp.sqrt(jnp.float32(C))
    scores = jnp.einsum('qc,kc->qk', queries.astype(jnp.float32), key_rows.astype(jnp.float32)) * scaling
    rowmax = lax.optimization_barrier(jnp.max(scores, axis=1))
    expo = jnp.exp(scores - rowmax[:, None])
    denominator = lax.optimization_barrier(jnp.sum(expo, axis=1))
    probs = expo.astype(jnp.bfloat16)
    attended = (jnp.dot(probs, values, preferred_element_type=jnp.float32) / denominator[:, None]).astype(jnp.bfloat16)
    hidden = (positions.astype(jnp.float32) + jnp.dot(attended, w_out, preferred_element_type=jnp.float32)).astype(jnp.bfloat16)
    activated = jax.nn.silu(group_norm(hidden, conv_gain, conv_shift)).astype(jnp.bfloat16).reshape(H, W, C)
    padded = jnp.pad(activated, ((1, 1), (1, 1), (0, 0)))
    convolved = jnp.zeros((H * W, C), jnp.float32)
    for row_tap in range(3):
        for col_tap in range(3):
            window = padded[row_tap:row_tap + H, col_tap:col_tap + W].reshape(H * W, C)
            convolved = convolved + jnp.dot(window, w_conv[row_tap, col_tap], preferred_element_type=jnp.float32)
    encoded = hidden.astype(jnp.float32) + (convolved + conv_bias)
    return encoded.astype(jnp.bfloat16).reshape(H, W, C)
```

```python
import functools
import math

import jax
import jax.numpy as jnp
from jax import lax
from jax.experimental import pallas as pl
from jax.experimental.pallas import tpu as pltpu
from jax.sharding import PartitionSpec as P

GROUPS = 32
EPS = 1e-06
CHUNK = 128
MESH = pl.DeviceIdType.MESH
LOG2E = math.log2(math.e)
NT = (((1,), (1,)), ((), ()))


def spread_groups(row, ones):
    high = row.astype(jnp.bfloat16).astype(jnp.float32)
    rest = row - high
    mid = rest.astype(jnp.bfloat16).astype(jnp.float32)
    low = rest - mid
    index = lax.broadcasted_iota(jnp.int32, (16, row.shape[1]), 0)
    parts = jnp.where(index == 0, high, jnp.where(index == 1, mid, jnp.where(index == 2, low, 0.0)))
    sums = jnp.dot(parts.astype(jnp.bfloat16), ones, preferred_element_type=jnp.float32)
    return jnp.sum(sums, axis=0, keepdims=True)


def kernel(
    n, wide,
    latent, w_query, w_key, w_value, w_out, w_conv,
    attn_gain, attn_shift, conv_gain, conv_shift, conv_bias,
    out,
    kv, wq, wk, wv, wo, wc, ones, moments, queries, bias, maxima, total, acc, hidden, halo, stacked,
    load_sem, weight_sem, send_sem, recv_sem, stat_send, stat_recv, halo_send, halo_recv,
    result, store_sem,
):
    chunks, chunk, channels = kv.shape[1:]
    rows = chunks * chunk
    deep = n // 2
    far = deep // 2
    half_chunks = chunks // 2
    lines = rows // wide
    size = channels // GROUPS
    img = lax.axis_index("img")
    r = lax.axis_index("row")
    z = r // 2
    c = r % 2
    partner = r + 1 - 2 * c

    loads = [
        pltpu.make_async_copy(latent.at[k], kv.at[r, k], load_sem.at[k]) for k in range(chunks)
    ]
    for load in loads:
        load.start()
    weights = [
        pltpu.make_async_copy(source, target, weight_sem.at[i])
        for i, (source, target) in enumerate([(w_query, wq), (w_key, wk), (w_value, wv), (w_out, wo)])
    ]
    weights += [
        pltpu.make_async_copy(
            w_conv.at[dy, dx],
            wc.at[dx, pl.ds(dy * channels, channels)],
            weight_sem.at[4 + dy * 3 + dx],
        )
        for dy in range(3)
        for dx in range(3)
    ]
    for weight in weights:
        weight.start()

    barrier = pltpu.get_barrier_semaphore()

    @pl.loop(1, n)
    def _(j):
        pl.semaphore_signal(
            barrier, inc=1, device_id=(img, lax.rem(r + j, n)), device_id_type=MESH
        )

    def piece(way, zb, k):
        b = zb * 2 + c
        target = (lax.rem(r + 2, n), lax.rem(r + n - 2, n), partner)[way]
        return pltpu.make_async_remote_copy(
            src_ref=kv.at[b, k],
            dst_ref=kv.at[b, k],
            send_sem=send_sem.at[way, zb, k],
            recv_sem=recv_sem.at[b, k],
            device_id=(img, target),
            device_id_type=MESH,
        )

    def arrival(b, k):
        return pltpu.make_async_remote_copy(
            src_ref=kv.at[b, k],
            dst_ref=kv.at[b, k],
            send_sem=send_sem.at[0, 0, 0],
            recv_sem=recv_sem.at[b, k],
            device_id=(img, partner),
            device_id_type=MESH,
        )

    def stat_copy(which, j):
        return pltpu.make_async_remote_copy(
            src_ref=moments.at[which, r],
            dst_ref=moments.at[which, r],
            send_sem=stat_send.at[which, j],
            recv_sem=stat_recv.at[which, r],
            device_id=(img, lax.rem(r + j, n)),
            device_id_type=MESH,
        )

    def stat_arrival(which, b):
        return pltpu.make_async_remote_copy(
            src_ref=moments.at[which, b],
            dst_ref=moments.at[which, b],
            send_sem=stat_send.at[which, 0],
            recv_sem=stat_recv.at[which, b],
            device_id=(img, partner),
            device_id_type=MESH,
        )

    def send_own(k):
        piece(0, z, k).start()
        piece(1, z, k).start()
        piece(2, z, k).start()

    def share_moments(which, field):
        mean = jnp.sum(field, axis=0, keepdims=True) * (1.0 / rows)
        offset = field - mean
        square = jnp.sum(offset * offset, axis=0, keepdims=True)
        moments[which, r, 0:1, :] = mean
        moments[which, r, 1:2, :] = square

        @pl.loop(1, n)
        def _(j):
            stat_copy(which, j).start()

    def gather_moments(which):
        @pl.loop(1, n)
        def _(j):
            stat_arrival(which, lax.rem(r + j, n)).wait_recv()

        @pl.loop(1, n)
        def _(j):
            stat_copy(which, j).wait_send()

        every = moments[which]
        means = every[:, 0, :]
        squares = every[:, 1, :]
        centre = spread_groups(jnp.sum(means, axis=0, keepdims=True), ones[...]) * (
            1.0 / (n * size)
        )
        away = means - centre
        whole = jnp.sum(squares + rows * (away * away), axis=0, keepdims=True)
        variance = spread_groups(whole, ones[...]) * (1.0 / (n * size * rows))
        return centre, lax.rsqrt(variance + EPS)

    for load in loads:
        load.wait()
    pl.semaphore_wait(barrier, n - 1)
    send_own(0)
    share_moments(0, kv[r].reshape(rows, channels).astype(jnp.float32))
    for k in range(1, chunks):
        send_own(k)

    left_group = lax.broadcasted_iota(jnp.int32, (channels, channels), 0) // size
    right_group = lax.broadcasted_iota(jnp.int32, (channels, channels), 1) // size
    ones[...] = jnp.where(left_group == right_group, 1.0, 0.0).astype(jnp.bfloat16)
    maxima[...] = jnp.full_like(maxima, -1e30)
    total[...] = jnp.zeros_like(total)
    acc[...] = jnp.zeros_like(acc)

    for weight in weights[:2]:
        weight.wait()
    centre, scale = gather_moments(0)
    gain = scale * attn_gain[...]
    positions = kv[r].reshape(rows, channels).astype(jnp.float32)
    normed = ((positions - centre) * gain + attn_shift[...]).astype(jnp.bfloat16)
    query = jnp.dot(normed, wq[...], preferred_element_type=jnp.float32).astype(jnp.bfloat16)
    folded = lax.dot_general(query, wk[...], NT, preferred_element_type=jnp.float32) * (
        LOG2E / math.sqrt(channels)
    )
    queries[...] = (folded * gain).astype(jnp.bfloat16)
    constant = jnp.sum(folded * (attn_shift[...] - centre * gain), axis=1, keepdims=True)
    bias[...] = jnp.broadcast_to(constant, bias.shape)

    def attend(b, k):
        block = kv[b, k]
        scores = lax.dot_general(queries[...], block, NT, preferred_element_type=jnp.float32)
        scores = scores + jnp.tile(bias[...], (1, chunk // 128))
        newest = jnp.maximum(maxima[...], jnp.max(scores, axis=1, keepdims=True))
        fade = jnp.exp2(maxima[...] - newest)
        maxima[...] = newest
        probs = jnp.exp2(scores - jnp.tile(newest, (1, chunk // 128))).astype(jnp.bfloat16)
        kept = probs.astype(jnp.float32)
        summed = total[...] * fade
        for j in range(chunk // 128):
            summed = summed + kept[:, j * 128 : (j + 1) * 128]
        total[...] = summed
        product = jnp.dot(probs, block, preferred_element_type=jnp.float32)
        acc[...] = acc[...] * jnp.tile(fade, (1, channels // 128)) + product

    def split(way, d, k):
        whole = d < far
        part = jnp.logical_and(d == far, (k < half_chunks) if way == 0 else (k >= half_chunks))
        return jnp.logical_or(whole, part)

    def relay(t):
        d = t // chunks
        k = t % chunks
        for way in (0, 1):
            zb = lax.rem(z + (deep - d if way == 0 else d), deep)

            @pl.when(split(way, d, k))
            def _(way=way, zb=zb):
                arrival(zb * 2 + c, k).wait_recv()

                @pl.when(split(way, d + 1, k))
                def _():
                    piece(way, zb, k).start()

                piece(2, zb, k).start()

    @pl.loop(0, (far + 1) * chunks)
    def _(t):
        d = t // chunks
        k = t % chunks

        @pl.when(t < chunks)
        def _():
            relay(t + chunks)

        @pl.when(t >= 2 * chunks)
        def _():
            relay(t)

        @pl.loop(0, 4)
        def _(j):
            side = j % 2
            other = j // 2
            zb = lax.rem(z + jnp.where(side == 0, deep - d, d), deep)
            mine = jnp.where(side == 0, split(0, d, k), split(1, d, k))

            @pl.when(jnp.logical_and(mine, jnp.logical_or(side == 0, d > 0)))
            def _():
                b = zb * 2 + c + other * (1 - 2 * c)

                @pl.when(other == 1)
                def _():
                    arrival(b, k).wait_recv()

                attend(b, k)

    for weight in weights[2:4]:
        weight.wait()
    denominator = jnp.sum(total[...], axis=1, keepdims=True)
    average = (acc[...] / denominator - centre) * gain + attn_shift[...]
    attended = jnp.dot(
        average.astype(jnp.bfloat16), wv[...], preferred_element_type=jnp.float32
    ).astype(jnp.bfloat16)
    field = (
        kv[r].reshape(rows, channels).astype(jnp.float32)
        + jnp.dot(attended, wo[...], preferred_element_type=jnp.float32)
    ).astype(jnp.bfloat16)
    hidden[...] = field
    share_moments(1, field.astype(jnp.float32))

    up = pltpu.make_async_remote_copy(
        src_ref=hidden.at[pl.ds(0, wide)],
        dst_ref=halo.at[1],
        send_sem=halo_send.at[1],
        recv_sem=halo_recv.at[1],
        device_id=(img, r - 1),
        device_id_type=MESH,
    )
    down = pltpu.make_async_remote_copy(
        src_ref=hidden.at[pl.ds(rows - wide, wide)],
        dst_ref=halo.at[0],
        send_sem=halo_send.at[0],
        recv_sem=halo_recv.at[0],
        device_id=(img, r + 1),
        device_id_type=MESH,
    )

    @pl.when(r > 0)
    def _():
        up.start()

    @pl.when(r < n - 1)
    def _():
        down.start()

    @pl.loop(0, deep * chunks)
    def _(t):
        zb = t // chunks
        k = t % chunks

        @pl.when(split(0, lax.rem(z + deep - zb, deep) + 1, k))
        def _():
            piece(0, zb, k).wait_send()

        @pl.when(split(1, lax.rem(zb + deep - z, deep) + 1, k))
        def _():
            piece(1, zb, k).wait_send()

        piece(2, zb, k).wait_send()

    for weight in weights[4:]:
        weight.wait()
    centre, scale = gather_moments(1)
    gain = scale * conv_gain[...]

    def activate(values):
        v = (values.astype(jnp.float32) - centre) * gain + conv_shift[...]
        return (v / (1.0 + jnp.exp(-v))).astype(jnp.bfloat16)

    def place(line, values):
        for dy in range(3):
            y = line + 1 - dy
            if 0 <= y < lines:
                stacked[y * wide : (y + 1) * wide, dy * channels : (dy + 1) * channels] = values

    for line in range(lines):
        place(line, activate(hidden[line * wide : (line + 1) * wide]))

    @pl.when(r > 0)
    def _():
        up.wait_send()
        down.wait_recv()
        place(-1, activate(halo[0]))

    @pl.when(r == 0)
    def _():
        place(-1, jnp.zeros((wide, channels), jnp.bfloat16))

    @pl.when(r < n - 1)
    def _():
        down.wait_send()
        up.wait_recv()
        place(lines, activate(halo[1]))

    @pl.when(r == n - 1)
    def _():
        place(lines, jnp.zeros((wide, channels), jnp.bfloat16))

    half = 256
    stores = []
    column = lax.broadcasted_iota(jnp.int32, (rows, half), 0) % wide
    for start in range(0, channels, half):
        cut = slice(start, start + half)

        def taps(dx):
            return jnp.dot(stacked[...], wc[dx, :, cut], preferred_element_type=jnp.float32)

        convolved = taps(1)
        convolved = convolved + jnp.where(column > 0, pltpu.roll(taps(0), 1, 0), 0.0)
        convolved = convolved + jnp.where(
            column < wide - 1, pltpu.roll(taps(2), rows - 1, 0), 0.0
        )
        encoded = hidden[:, cut].astype(jnp.float32) + (convolved + conv_bias[:, cut])
        result[:, cut] = encoded.astype(jnp.bfloat16)
        store = pltpu.make_async_copy(
            result.at[:, cut], out.at[:, cut], store_sem.at[start // half]
        )
        store.start()
        stores.append(store)

    for store in stores:
        store.wait()


def local(n, latent, attn_gain, attn_shift, w_query, w_key, w_value, w_out,
          conv_gain, conv_shift, w_conv, conv_bias):
    height, wide, channels = latent.shape
    rows = height * wide
    chunks = rows // CHUNK
    anywhere = pl.BlockSpec(memory_space=pl.ANY)
    vmem = pl.BlockSpec(memory_space=pltpu.VMEM)
    bf16, f32 = jnp.bfloat16, jnp.float32
    square = pltpu.VMEM((channels, channels), bf16)
    dma = pltpu.SemaphoreType.DMA
    encoded = pl.pallas_call(
        functools.partial(kernel, n, wide),
        out_shape=jax.ShapeDtypeStruct((rows, channels), bf16),
        in_specs=[anywhere] * 6 + [vmem] * 5,
        out_specs=anywhere,
        scratch_shapes=[
            pltpu.VMEM((n, chunks, CHUNK, channels), bf16),
            square, square, square, square,
            pltpu.VMEM((3, 3 * channels, channels), bf16),
            square,
            pltpu.VMEM((2, n, 2, channels), f32),
            pltpu.VMEM((rows, channels), bf16),
            pltpu.VMEM((rows, 128), f32),
            pltpu.VMEM((rows, 128), f32),
            pltpu.VMEM((rows, 128), f32),
            pltpu.VMEM((rows, channels), f32),
            pltpu.VMEM((rows, channels), bf16),
            pltpu.VMEM((2, wide, channels), bf16),
            pltpu.VMEM((rows, 3 * channels), bf16),
            dma((chunks,)),
            dma((13,)),
            dma((3, n // 2, chunks)),
            dma((n, chunks)),
            dma((2, n)),
            dma((2, n)),
            dma((2,)),
            dma((2,)),
            pltpu.VMEM((rows, channels), bf16),
            dma((channels // 256,)),
        ],
        compiler_params=pltpu.CompilerParams(
            collective_id=0, has_side_effects=True, vmem_limit_bytes=56 * 1024 * 1024
        ),
    )(
        latent.reshape(chunks, CHUNK, channels), w_query, w_key, w_value, w_out, w_conv,
        *(v.reshape(1, channels) for v in (attn_gain, attn_shift, conv_gain, conv_shift, conv_bias)),
    )
    return encoded.reshape(height, wide, channels)


def solution(mesh):
    in_specs = (P(("img", "row"), None, None), P(), P(), P(), P(), P(), P(), P(), P(), P(), P())
    out_specs = P(("img", "row"), None, None)
    body = functools.partial(local, mesh.shape["row"])
    return jax.shard_map(body, mesh=mesh, in_specs=in_specs, out_specs=out_specs, check_vma=False)
```

```python
import functools
import math

import jax
import jax.numpy as jnp
from jax import lax
from jax.experimental import pallas as pl
from jax.experimental.pallas import tpu as pltpu
from jax.sharding import PartitionSpec as P

GROUPS = 32
EPS = 1e-06
CHUNK = 128
MESH = pl.DeviceIdType.MESH
LOG2E = math.log2(math.e)
NT = (((1,), (1,)), ((), ()))


def spread_groups(row, ones):
    high = row.astype(jnp.bfloat16).astype(jnp.float32)
    rest = row - high
    mid = rest.astype(jnp.bfloat16).astype(jnp.float32)
    low = rest - mid
    index = lax.broadcasted_iota(jnp.int32, (16, row.shape[1]), 0)
    parts = jnp.where(index == 0, high, jnp.where(index == 1, mid, jnp.where(index == 2, low, 0.0)))
    sums = jnp.dot(parts.astype(jnp.bfloat16), ones, preferred_element_type=jnp.float32)
    return jnp.sum(sums, axis=0, keepdims=True)


def kernel(
    n, wide,
    latent, w_query, w_key, w_value, w_out, w_conv,
    attn_gain, attn_shift, conv_gain, conv_shift, conv_bias,
    out,
    kv, wq, wk, wv, wo, wvo, wc, ones, moments, queries, bias, maxima, total, acc, hidden, halo, stacked,
    load_sem, weight_sem, send_sem, recv_sem, stat_send, stat_recv, halo_send, halo_recv,
    result, store_sem,
):
    deep, chunks, _, chunk, channels = kv.shape
    rows = chunks * chunk
    far = deep // 2
    half_chunks = chunks // 2
    lines = rows // wide
    size = channels // GROUPS
    img = lax.axis_index("img")
    r = lax.axis_index("row")
    z = r // 2
    c = r % 2
    partner = r + 1 - 2 * c

    loads = [
        pltpu.make_async_copy(latent.at[k], kv.at[z, k, c], load_sem.at[k]) for k in range(chunks)
    ]
    for load in loads:
        load.start()
    weights = [
        pltpu.make_async_copy(source, target, weight_sem.at[i])
        for i, (source, target) in enumerate([(w_query, wq), (w_key, wk), (w_value, wv), (w_out, wo)])
    ]
    weights += [
        pltpu.make_async_copy(
            w_conv.at[dy, dx],
            wc.at[dx, pl.ds(dy * channels, channels)],
            weight_sem.at[4 + dy * 3 + dx],
        )
        for dy in range(3)
        for dx in range(3)
    ]
    for weight in weights:
        weight.start()

    barrier = pltpu.get_barrier_semaphore()

    @pl.loop(1, n)
    def _(j):
        pl.semaphore_signal(
            barrier, inc=1, device_id=(img, lax.rem(r + j, n)), device_id_type=MESH
        )

    def piece(way, zb, k):
        target = (lax.rem(r + 2, n), lax.rem(r + n - 2, n), partner)[way]
        return pltpu.make_async_remote_copy(
            src_ref=kv.at[zb, k, c],
            dst_ref=kv.at[zb, k, c],
            send_sem=send_sem.at[way, zb, k],
            recv_sem=recv_sem.at[c, zb, k],
            device_id=(img, target),
            device_id_type=MESH,
        )

    def arrival(core, zb, k):
        return pltpu.make_async_remote_copy(
            src_ref=kv.at[zb, k, core],
            dst_ref=kv.at[zb, k, core],
            send_sem=send_sem.at[0, 0, 0],
            recv_sem=recv_sem.at[core, zb, k],
            device_id=(img, partner),
            device_id_type=MESH,
        )

    def stat_copy(which, j):
        return pltpu.make_async_remote_copy(
            src_ref=moments.at[which, r],
            dst_ref=moments.at[which, r],
            send_sem=stat_send.at[which, j],
            recv_sem=stat_recv.at[which, r],
            device_id=(img, lax.rem(r + j, n)),
            device_id_type=MESH,
        )

    def stat_arrival(which, b):
        return pltpu.make_async_remote_copy(
            src_ref=moments.at[which, b],
            dst_ref=moments.at[which, b],
            send_sem=stat_send.at[which, 0],
            recv_sem=stat_recv.at[which, b],
            device_id=(img, partner),
            device_id_type=MESH,
        )

    def own():
        return kv[z, :, c]

    def send_own(k):
        piece(0, z, k).start()
        piece(1, z, k).start()
        piece(2, z, k).start()

    def share_moments(which, field):
        mean = jnp.sum(field, axis=0, keepdims=True) * (1.0 / rows)
        offset = field - mean
        square = jnp.sum(offset * offset, axis=0, keepdims=True)
        moments[which, r, 0:1, :] = mean
        moments[which, r, 1:2, :] = square

        @pl.loop(1, n)
        def _(j):
            stat_copy(which, j).start()

    def gather_moments(which):
        @pl.loop(1, n)
        def _(j):
            stat_arrival(which, lax.rem(r + j, n)).wait_recv()

        @pl.loop(1, n)
        def _(j):
            stat_copy(which, j).wait_send()

        every = moments[which]
        means = every[:, 0, :]
        squares = every[:, 1, :]
        centre = spread_groups(jnp.sum(means, axis=0, keepdims=True), ones[...]) * (
            1.0 / (n * size)
        )
        away = means - centre
        whole = jnp.sum(squares + rows * (away * away), axis=0, keepdims=True)
        variance = spread_groups(whole, ones[...]) * (1.0 / (n * size * rows))
        return centre, lax.rsqrt(variance + EPS)

    for load in loads:
        load.wait()
    pl.semaphore_wait(barrier, n - 1)
    send_own(0)
    share_moments(0, own().reshape(rows, channels).astype(jnp.float32))
    for k in range(1, chunks):
        send_own(k)

    left_group = lax.broadcasted_iota(jnp.int32, (channels, channels), 0) // size
    right_group = lax.broadcasted_iota(jnp.int32, (channels, channels), 1) // size
    ones[...] = jnp.where(left_group == right_group, 1.0, 0.0).astype(jnp.bfloat16)
    maxima[...] = jnp.full_like(maxima, -1e30)
    total[...] = jnp.zeros_like(total)
    acc[...] = jnp.zeros_like(acc)

    for weight in weights[:2]:
        weight.wait()
    centre, scale = gather_moments(0)
    gain = scale * attn_gain[...]
    positions = own().reshape(rows, channels).astype(jnp.float32)
    normed = ((positions - centre) * gain + attn_shift[...]).astype(jnp.bfloat16)
    query = jnp.dot(normed, wq[...], preferred_element_type=jnp.float32).astype(jnp.bfloat16)
    folded = lax.dot_general(query, wk[...], NT, preferred_element_type=jnp.float32) * (
        LOG2E / math.sqrt(channels)
    )
    queries[...] = (folded * gain).astype(jnp.bfloat16)
    constant = jnp.sum(folded * (attn_shift[...] - centre * gain), axis=1, keepdims=True)
    bias[...] = jnp.broadcast_to(constant, bias.shape)

    for weight in weights[2:4]:
        weight.wait()
    wvo[...] = jnp.dot(wv[...], wo[...], preferred_element_type=jnp.float32).astype(jnp.bfloat16)

    lanes = 128
    halves = [slice(i, i + rows // 2) for i in range(0, rows, rows // 2)]

    def attend(places):
        blocks = [kv[zb, k].reshape(2 * chunk, channels) for zb, k in places]
        scores = [
            [
                lax.dot_general(queries[part], block, NT, preferred_element_type=jnp.float32)
                for block in blocks
            ]
            for part in halves
        ]
        for part, pair in zip(halves, scores):
            columns = [
                score[:, j : j + lanes] for score in pair for j in range(0, 2 * chunk, lanes)
            ]
            peak = functools.reduce(jnp.maximum, columns)
            offset = bias[part]
            newest = jnp.maximum(maxima[part], jnp.max(peak, axis=1, keepdims=True) + offset)
            fade = jnp.exp2(maxima[part] - newest)
            maxima[part] = newest
            level = newest - offset
            weights = [jnp.exp2(column - level) for column in columns]
            total[part] = functools.reduce(jnp.add, weights, total[part] * fade)
            each = len(weights) // 2
            product = 0.0
            for i, block in enumerate(blocks):
                probs = jnp.concatenate(weights[i * each : (i + 1) * each], axis=1)
                product = product + jnp.dot(
                    probs.astype(jnp.bfloat16), block, preferred_element_type=jnp.float32
                )
            acc[part] = acc[part] * jnp.tile(fade, (1, channels // lanes)) + product

    def split(way, d, k):
        part = (k < half_chunks) if way == 0 else (k >= half_chunks)
        return jnp.logical_or(d < far, jnp.logical_and(d == far, part))

    own_steps = half_chunks

    def spot(way, s):
        e = s - own_steps
        d = jnp.where(e < 0, 0, e // chunks + 1)
        last = d == far
        step = jnp.where(e < 0, 2 * s + way, lax.rem(e + chunks, chunks) + jnp.where(last, way * half_chunks, 0))
        zb = lax.rem(z + (deep - d if way == 0 else d), deep)
        return d, zb, step

    def relay(s):
        for way in (0, 1):
            d, zb, k = spot(way, s)
            arrival(c, zb, k).wait_recv()

            @pl.when(split(way, d + 1, k))
            def _(way=way, zb=zb, k=k):
                piece(way, zb, k).start()

            piece(2, zb, k).start()

    ahead = 2
    steps = own_steps + (far - 1) * chunks + half_chunks
    for s in range(own_steps, own_steps + ahead):
        relay(s)

    @pl.loop(0, steps)
    def _(s):
        @pl.when(s >= own_steps + ahead)
        def _():
            relay(s)

        places = []
        for way in (0, 1):
            d, zb, k = spot(way, s)
            arrival(1 - c, zb, k).wait_recv()
            places.append((zb, k))
        attend(places)

    denominator = jnp.sum(total[...], axis=1, keepdims=True)
    average = (acc[...] * (1.0 / denominator) - centre) * gain + attn_shift[...]
    attended = jnp.dot(
        average.astype(jnp.bfloat16), wvo[...], preferred_element_type=jnp.float32
    )
    field = (own().reshape(rows, channels).astype(jnp.float32) + attended).astype(jnp.bfloat16)
    hidden[...] = field
    share_moments(1, field.astype(jnp.float32))

    up = pltpu.make_async_remote_copy(
        src_ref=hidden.at[pl.ds(0, wide)],
        dst_ref=halo.at[1],
        send_sem=halo_send.at[1],
        recv_sem=halo_recv.at[1],
        device_id=(img, r - 1),
        device_id_type=MESH,
    )
    down = pltpu.make_async_remote_copy(
        src_ref=hidden.at[pl.ds(rows - wide, wide)],
        dst_ref=halo.at[0],
        send_sem=halo_send.at[0],
        recv_sem=halo_recv.at[0],
        device_id=(img, r + 1),
        device_id_type=MESH,
    )

    @pl.when(r > 0)
    def _():
        up.start()

    @pl.when(r < n - 1)
    def _():
        down.start()

    @pl.loop(0, deep * chunks)
    def _(t):
        zb = t // chunks
        k = t % chunks

        @pl.when(split(0, lax.rem(z + deep - zb, deep) + 1, k))
        def _():
            piece(0, zb, k).wait_send()

        @pl.when(split(1, lax.rem(zb + deep - z, deep) + 1, k))
        def _():
            piece(1, zb, k).wait_send()

        piece(2, zb, k).wait_send()

    for weight in weights[4:]:
        weight.wait()
    centre, scale = gather_moments(1)
    gain = scale * conv_gain[...]

    def activate(values):
        v = (values.astype(jnp.float32) - centre) * gain + conv_shift[...]
        return (v / (1.0 + jnp.exp(-v))).astype(jnp.bfloat16)

    def place(line, values):
        for dy in range(3):
            y = line + 1 - dy
            if 0 <= y < lines:
                stacked[y * wide : (y + 1) * wide, dy * channels : (dy + 1) * channels] = values

    for line in range(lines):
        place(line, activate(hidden[line * wide : (line + 1) * wide]))

    @pl.when(r > 0)
    def _():
        up.wait_send()
        down.wait_recv()
        place(-1, activate(halo[0]))

    @pl.when(r == 0)
    def _():
        place(-1, jnp.zeros((wide, channels), jnp.bfloat16))

    @pl.when(r < n - 1)
    def _():
        down.wait_send()
        up.wait_recv()
        place(lines, activate(halo[1]))

    @pl.when(r == n - 1)
    def _():
        place(lines, jnp.zeros((wide, channels), jnp.bfloat16))

    half = 256
    stores = []
    column = lax.broadcasted_iota(jnp.int32, (rows, half), 0) % wide
    for start in range(0, channels, half):
        cut = slice(start, start + half)

        def taps(dx):
            return jnp.dot(stacked[...], wc[dx, :, cut], preferred_element_type=jnp.float32)

        convolved = taps(1)
        convolved = convolved + jnp.where(column > 0, pltpu.roll(taps(0), 1, 0), 0.0)
        convolved = convolved + jnp.where(
            column < wide - 1, pltpu.roll(taps(2), rows - 1, 0), 0.0
        )
        encoded = hidden[:, cut].astype(jnp.float32) + (convolved + conv_bias[:, cut])
        result[:, cut] = encoded.astype(jnp.bfloat16)
        store = pltpu.make_async_copy(
            result.at[:, cut], out.at[:, cut], store_sem.at[start // half]
        )
        store.start()
        stores.append(store)

    for store in stores:
        store.wait()


def local(n, latent, attn_gain, attn_shift, w_query, w_key, w_value, w_out,
          conv_gain, conv_shift, w_conv, conv_bias):
    height, wide, channels = latent.shape
    rows = height * wide
    chunks = rows // CHUNK
    anywhere = pl.BlockSpec(memory_space=pl.ANY)
    vmem = pl.BlockSpec(memory_space=pltpu.VMEM)
    bf16, f32 = jnp.bfloat16, jnp.float32
    square = pltpu.VMEM((channels, channels), bf16)
    dma = pltpu.SemaphoreType.DMA
    encoded = pl.pallas_call(
        functools.partial(kernel, n, wide),
        out_shape=jax.ShapeDtypeStruct((rows, channels), bf16),
        in_specs=[anywhere] * 6 + [vmem] * 5,
        out_specs=anywhere,
        scratch_shapes=[
            pltpu.VMEM((n // 2, chunks, 2, CHUNK, channels), bf16),
            square, square, square, square, square,
            pltpu.VMEM((3, 3 * channels, channels), bf16),
            square,
            pltpu.VMEM((2, n, 2, channels), f32),
            pltpu.VMEM((rows, channels), bf16),
            pltpu.VMEM((rows, 128), f32),
            pltpu.VMEM((rows, 128), f32),
            pltpu.VMEM((rows, 128), f32),
            pltpu.VMEM((rows, channels), f32),
            pltpu.VMEM((rows, channels), bf16),
            pltpu.VMEM((2, wide, channels), bf16),
            pltpu.VMEM((rows, 3 * channels), bf16),
            dma((chunks,)),
            dma((13,)),
            dma((3, n // 2, chunks)),
            dma((2, n // 2, chunks)),
            dma((2, n)),
            dma((2, n)),
            dma((2,)),
            dma((2,)),
            pltpu.VMEM((rows, channels), bf16),
            dma((channels // 256,)),
        ],
        compiler_params=pltpu.CompilerParams(
            collective_id=0, has_side_effects=True, vmem_limit_bytes=56 * 1024 * 1024
        ),
    )(
        latent.reshape(chunks, CHUNK, channels), w_query, w_key, w_value, w_out, w_conv,
        *(v.reshape(1, channels) for v in (attn_gain, attn_shift, conv_gain, conv_shift, conv_bias)),
    )
    return encoded.reshape(height, wide, channels)


def solution(mesh):
    in_specs = (P(("img", "row"), None, None), P(), P(), P(), P(), P(), P(), P(), P(), P(), P())
    out_specs = P(("img", "row"), None, None)
    body = functools.partial(local, mesh.shape["row"])
    return jax.shard_map(body, mesh=mesh, in_specs=in_specs, out_specs=out_specs, check_vma=False)
```

```python
import functools
import math

import jax
import jax.numpy as jnp
from jax import lax
from jax.experimental import pallas as pl
from jax.experimental.pallas import tpu as pltpu
from jax.sharding import PartitionSpec as P

GROUPS = 32
EPS = 1e-06
CHUNK = 128
MESH = pl.DeviceIdType.MESH
LOG2E = math.log2(math.e)
NT = (((1,), (1,)), ((), ()))


def spread_groups(row, ones):
    high = row.astype(jnp.bfloat16).astype(jnp.float32)
    rest = row - high
    mid = rest.astype(jnp.bfloat16).astype(jnp.float32)
    low = rest - mid
    index = lax.broadcasted_iota(jnp.int32, (16, row.shape[1]), 0)
    parts = jnp.where(index == 0, high, jnp.where(index == 1, mid, jnp.where(index == 2, low, 0.0)))
    sums = jnp.dot(parts.astype(jnp.bfloat16), ones, preferred_element_type=jnp.float32)
    return jnp.sum(sums, axis=0, keepdims=True)


def kernel(
    n, wide,
    latent, w_query, w_key, w_value, w_out, w_conv,
    attn_gain_in, attn_shift_in, conv_gain_in, conv_shift_in, conv_bias_in,
    out,
    kv, wq, wk, wv, wo, wvo, wc, ones, moments, queries, bias, maxima, total, acc, hidden, halo, stacked,
    load_sem, weight_sem, send_sem, recv_sem, stat_send, stat_recv, halo_send, halo_recv,
    result, store_sem, vectors, vector_sem, entered,
):
    deep, chunks, _, chunk, channels = kv.shape
    rows = chunks * chunk
    far = deep // 2
    half_chunks = chunks // 2
    early = 2
    lines = rows // wide
    size = channels // GROUPS
    img = lax.axis_index("img")
    r = lax.axis_index("row")
    z = r // 2
    c = r % 2
    partner = r + 1 - 2 * c

    barrier = pltpu.get_barrier_semaphore()

    upward, downward = lax.rem(r + 2, n), lax.rem(r + n - 2, n)
    for target in (upward, downward, partner):
        pl.semaphore_signal(barrier, inc=1, device_id=(img, target), device_id_type=MESH)

    loads = [
        pltpu.make_async_copy(latent.at[k], kv.at[z, k, c], load_sem.at[k]) for k in range(chunks)
    ]
    for load in loads:
        load.start()
    weights = [
        pltpu.make_async_copy(source, target, weight_sem.at[i])
        for i, (source, target) in enumerate([(w_query, wq), (w_key, wk), (w_value, wv), (w_out, wo)])
    ]
    weights += [
        pltpu.make_async_copy(
            w_conv.at[dy, dx],
            wc.at[dx, pl.ds(dy * channels, channels)],
            weight_sem.at[4 + dy * 3 + dx],
        )
        for dy in range(3)
        for dx in range(3)
    ]
    for weight in weights:
        weight.start()

    small = [
        pltpu.make_async_copy(source, vectors.at[pl.ds(i, 1)], vector_sem.at[i])
        for i, source in enumerate(
            [attn_gain_in, attn_shift_in, conv_gain_in, conv_shift_in, conv_bias_in]
        )
    ]
    for copy in small:
        copy.start()

    def piece(way, zb, k):
        target = (upward, downward, partner)[way]
        return pltpu.make_async_remote_copy(
            src_ref=kv.at[zb, k, c],
            dst_ref=kv.at[zb, k, c],
            send_sem=send_sem.at[way, zb, k],
            recv_sem=recv_sem.at[c, zb, k],
            device_id=(img, target),
            device_id_type=MESH,
        )

    def arrival(core, zb, k):
        return pltpu.make_async_remote_copy(
            src_ref=kv.at[zb, k, core],
            dst_ref=kv.at[zb, k, core],
            send_sem=send_sem.at[0, 0, 0],
            recv_sem=recv_sem.at[core, zb, k],
            device_id=(img, partner),
            device_id_type=MESH,
        )

    def stat_copy(which, j):
        return pltpu.make_async_remote_copy(
            src_ref=moments.at[which, r],
            dst_ref=moments.at[which, r],
            send_sem=stat_send.at[which, j],
            recv_sem=stat_recv.at[which, r],
            device_id=(img, lax.rem(r + j, n)),
            device_id_type=MESH,
        )

    def stat_arrival(which, b):
        return pltpu.make_async_remote_copy(
            src_ref=moments.at[which, b],
            dst_ref=moments.at[which, b],
            send_sem=stat_send.at[which, 0],
            recv_sem=stat_recv.at[which, b],
            device_id=(img, partner),
            device_id_type=MESH,
        )

    def own():
        return kv[z, :, c]

    def send_own(k):
        piece(0, z, k).start()
        piece(1, z, k).start()
        piece(2, z, k).start()

    def share_moments(which, field):
        mean = jnp.sum(field, axis=0, keepdims=True) * (1.0 / rows)
        offset = field - mean
        square = jnp.sum(offset * offset, axis=0, keepdims=True)
        moments[which, r, 0:1, :] = mean
        moments[which, r, 1:2, :] = square

        @pl.loop(1, n)
        def _(j):
            stat_copy(which, j).start()

    def gather_moments(which):
        @pl.loop(1, n)
        def _(j):
            stat_arrival(which, lax.rem(r + j, n)).wait_recv()

        @pl.loop(1, n)
        def _(j):
            stat_copy(which, j).wait_send()

        every = moments[which]
        means = every[:, 0, :]
        squares = every[:, 1, :]
        centre = spread_groups(jnp.sum(means, axis=0, keepdims=True), ones[...]) * (
            1.0 / (n * size)
        )
        away = means - centre
        whole = jnp.sum(squares + rows * (away * away), axis=0, keepdims=True)
        variance = spread_groups(whole, ones[...]) * (1.0 / (n * size * rows))
        return centre, lax.rsqrt(variance + EPS)

    pl.semaphore_wait(barrier, 3)
    for k in range(chunks):
        loads[k].wait()
        if k < early:
            send_own(k)
    for j in range(far - 1):
        for target in (upward, downward):
            pl.semaphore_signal(
                entered.at[j], inc=1, device_id=(img, target), device_id_type=MESH
            )
        pl.semaphore_wait(entered.at[j], 2)
    pl.semaphore_signal(entered.at[far - 1], inc=1, device_id=(img, partner), device_id_type=MESH)
    pl.semaphore_wait(entered.at[far - 1], 1)
    share_moments(0, own().reshape(rows, channels).astype(jnp.float32))
    for k in range(early, chunks):
        send_own(k)

    left_group = lax.broadcasted_iota(jnp.int32, (channels, channels), 0) // size
    right_group = lax.broadcasted_iota(jnp.int32, (channels, channels), 1) // size
    ones[...] = jnp.where(left_group == right_group, 1.0, 0.0).astype(jnp.bfloat16)
    maxima[...] = jnp.full_like(maxima, -1e30)
    total[...] = jnp.zeros_like(total)
    acc[...] = jnp.zeros_like(acc)

    for weight in weights[:2]:
        weight.wait()
    for copy in small:
        copy.wait()
    attn_gain, attn_shift, conv_gain, conv_shift = (vectors[i : i + 1] for i in range(4))
    conv_bias = vectors.at[4:5]
    centre, scale = gather_moments(0)
    gain = scale * attn_gain
    positions = own().reshape(rows, channels).astype(jnp.float32)
    normed = ((positions - centre) * gain + attn_shift).astype(jnp.bfloat16)
    query = jnp.dot(normed, wq[...], preferred_element_type=jnp.float32).astype(jnp.bfloat16)
    folded = lax.dot_general(query, wk[...], NT, preferred_element_type=jnp.float32) * (
        LOG2E / math.sqrt(channels)
    )
    queries[...] = (folded * gain).astype(jnp.bfloat16)
    constant = jnp.sum(folded * (attn_shift - centre * gain), axis=1, keepdims=True)
    bias[...] = jnp.broadcast_to(constant, bias.shape)

    for weight in weights[2:4]:
        weight.wait()
    wvo[...] = jnp.dot(wv[...], wo[...], preferred_element_type=jnp.float32).astype(jnp.bfloat16)

    lanes = 128
    halves = [slice(i, i + rows // 2) for i in range(0, rows, rows // 2)]

    def attend(places):
        blocks = [kv[zb, k].reshape(2 * chunk, channels) for zb, k in places]
        scores = [
            [
                lax.dot_general(queries[part], block, NT, preferred_element_type=jnp.float32)
                for block in blocks
            ]
            for part in halves
        ]
        for part, pair in zip(halves, scores):
            columns = [
                score[:, j : j + lanes] for score in pair for j in range(0, 2 * chunk, lanes)
            ]
            peak = functools.reduce(jnp.maximum, columns)
            offset = bias[part]
            newest = jnp.maximum(maxima[part], jnp.max(peak, axis=1, keepdims=True) + offset)
            fade = jnp.exp2(maxima[part] - newest)
            maxima[part] = newest
            level = newest - offset
            weights = [jnp.exp2(column - level) for column in columns]
            total[part] = functools.reduce(jnp.add, weights, total[part] * fade)
            each = len(weights) // 2
            product = 0.0
            for i, block in enumerate(blocks):
                probs = jnp.concatenate(weights[i * each : (i + 1) * each], axis=1)
                product = product + jnp.dot(
                    probs.astype(jnp.bfloat16), block, preferred_element_type=jnp.float32
                )
            acc[part] = acc[part] * jnp.tile(fade, (1, channels // lanes)) + product

    def split(way, d, k):
        part = (k < half_chunks) if way == 0 else (k >= half_chunks)
        return jnp.logical_or(d < far, jnp.logical_and(d == far, part))

    own_steps = half_chunks

    def spot(way, s):
        e = s - own_steps
        d = jnp.where(e < 0, 0, e // chunks + 1)
        last = d == far
        step = jnp.where(e < 0, 2 * s + way, lax.rem(e + chunks, chunks) + jnp.where(last, way * half_chunks, 0))
        zb = lax.rem(z + (deep - d if way == 0 else d), deep)
        return d, zb, step

    def relay(s):
        for way in (0, 1):
            d, zb, k = spot(way, s)
            arrival(c, zb, k).wait_recv()

            @pl.when(split(way, d + 1, k))
            def _(way=way, zb=zb, k=k):
                piece(way, zb, k).start()

            piece(2, zb, k).start()

    ahead = 2
    steps = own_steps + (far - 1) * chunks + half_chunks
    for s in range(own_steps, own_steps + ahead):
        relay(s)

    @pl.loop(0, steps)
    def _(s):
        @pl.when(s >= own_steps + ahead)
        def _():
            relay(s)

        places = []
        for way in (0, 1):
            d, zb, k = spot(way, s)
            arrival(1 - c, zb, k).wait_recv()
            places.append((zb, k))
        attend(places)

    denominator = jnp.sum(total[...], axis=1, keepdims=True)
    average = (acc[...] * (1.0 / denominator) - centre) * gain + attn_shift
    attended = jnp.dot(
        average.astype(jnp.bfloat16), wvo[...], preferred_element_type=jnp.float32
    )
    field = (own().reshape(rows, channels).astype(jnp.float32) + attended).astype(jnp.bfloat16)
    hidden[...] = field
    share_moments(1, field.astype(jnp.float32))

    up = pltpu.make_async_remote_copy(
        src_ref=hidden.at[pl.ds(0, wide)],
        dst_ref=halo.at[1],
        send_sem=halo_send.at[1],
        recv_sem=halo_recv.at[1],
        device_id=(img, r - 1),
        device_id_type=MESH,
    )
    down = pltpu.make_async_remote_copy(
        src_ref=hidden.at[pl.ds(rows - wide, wide)],
        dst_ref=halo.at[0],
        send_sem=halo_send.at[0],
        recv_sem=halo_recv.at[0],
        device_id=(img, r + 1),
        device_id_type=MESH,
    )

    @pl.when(r > 0)
    def _():
        up.start()

    @pl.when(r < n - 1)
    def _():
        down.start()

    @pl.loop(0, deep * chunks)
    def _(t):
        zb = t // chunks
        k = t % chunks

        @pl.when(split(0, lax.rem(z + deep - zb, deep) + 1, k))
        def _():
            piece(0, zb, k).wait_send()

        @pl.when(split(1, lax.rem(zb + deep - z, deep) + 1, k))
        def _():
            piece(1, zb, k).wait_send()

        piece(2, zb, k).wait_send()

    for weight in weights[4:]:
        weight.wait()
    centre, scale = gather_moments(1)
    gain = scale * conv_gain

    def activate(values):
        v = (values.astype(jnp.float32) - centre) * gain + conv_shift
        return (v / (1.0 + jnp.exp(-v))).astype(jnp.bfloat16)

    def place(line, values):
        for dy in range(3):
            y = line + 1 - dy
            if 0 <= y < lines:
                stacked[y * wide : (y + 1) * wide, dy * channels : (dy + 1) * channels] = values

    for line in range(lines):
        place(line, activate(hidden[line * wide : (line + 1) * wide]))

    @pl.when(r > 0)
    def _():
        up.wait_send()
        down.wait_recv()
        place(-1, activate(halo[0]))

    @pl.when(r == 0)
    def _():
        place(-1, jnp.zeros((wide, channels), jnp.bfloat16))

    @pl.when(r < n - 1)
    def _():
        down.wait_send()
        up.wait_recv()
        place(lines, activate(halo[1]))

    @pl.when(r == n - 1)
    def _():
        place(lines, jnp.zeros((wide, channels), jnp.bfloat16))

    half = 256
    stores = []
    column = lax.broadcasted_iota(jnp.int32, (rows, half), 0) % wide
    for start in range(0, channels, half):
        cut = slice(start, start + half)

        def taps(dx):
            return jnp.dot(stacked[...], wc[dx, :, cut], preferred_element_type=jnp.float32)

        convolved = taps(1)
        convolved = convolved + jnp.where(column > 0, pltpu.roll(taps(0), 1, 0), 0.0)
        convolved = convolved + jnp.where(
            column < wide - 1, pltpu.roll(taps(2), rows - 1, 0), 0.0
        )
        encoded = hidden[:, cut].astype(jnp.float32) + (convolved + conv_bias[:, cut])
        result[:, cut] = encoded.astype(jnp.bfloat16)
        store = pltpu.make_async_copy(
            result.at[:, cut], out.at[:, cut], store_sem.at[start // half]
        )
        store.start()
        stores.append(store)

    for store in stores:
        store.wait()


def local(n, latent, attn_gain, attn_shift, w_query, w_key, w_value, w_out,
          conv_gain, conv_shift, w_conv, conv_bias):
    height, wide, channels = latent.shape
    rows = height * wide
    chunks = rows // CHUNK
    anywhere = pl.BlockSpec(memory_space=pl.ANY)
    bf16, f32 = jnp.bfloat16, jnp.float32
    square = pltpu.VMEM((channels, channels), bf16)
    dma = pltpu.SemaphoreType.DMA
    encoded = pl.pallas_call(
        functools.partial(kernel, n, wide),
        out_shape=jax.ShapeDtypeStruct((rows, channels), bf16),
        in_specs=[anywhere] * 11,
        out_specs=anywhere,
        scratch_shapes=[
            pltpu.VMEM((n // 2, chunks, 2, CHUNK, channels), bf16),
            square, square, square, square, square,
            pltpu.VMEM((3, 3 * channels, channels), bf16),
            square,
            pltpu.VMEM((2, n, 2, channels), f32),
            pltpu.VMEM((rows, channels), bf16),
            pltpu.VMEM((rows, 128), f32),
            pltpu.VMEM((rows, 128), f32),
            pltpu.VMEM((rows, 128), f32),
            pltpu.VMEM((rows, channels), f32),
            pltpu.VMEM((rows, channels), bf16),
            pltpu.VMEM((2, wide, channels), bf16),
            pltpu.VMEM((rows, 3 * channels), bf16),
            dma((chunks,)),
            dma((13,)),
            dma((3, n // 2, chunks)),
            dma((2, n // 2, chunks)),
            dma((2, n)),
            dma((2, n)),
            dma((2,)),
            dma((2,)),
            pltpu.VMEM((rows, channels), bf16),
            dma((channels // 256,)),
            pltpu.VMEM((8, channels), f32),
            dma((5,)),
            pltpu.SemaphoreType.REGULAR((n // 4,)),
        ],
        compiler_params=pltpu.CompilerParams(
            collective_id=0, has_side_effects=True, vmem_limit_bytes=56 * 1024 * 1024
        ),
    )(
        latent.reshape(chunks, CHUNK, channels), w_query, w_key, w_value, w_out, w_conv,
        *(v.reshape(1, channels) for v in (attn_gain, attn_shift, conv_gain, conv_shift, conv_bias)),
    )
    return encoded.reshape(height, wide, channels)


def solution(mesh):
    in_specs = (P(("img", "row"), None, None), P(), P(), P(), P(), P(), P(), P(), P(), P(), P())
    out_specs = P(("img", "row"), None, None)
    body = functools.partial(local, mesh.shape["row"])
    return jax.shard_map(body, mesh=mesh, in_specs=in_specs, out_specs=out_specs, check_vma=False)
```

```python
import functools
import math

import jax
import jax.numpy as jnp
from jax import lax
from jax.experimental import pallas as pl
from jax.experimental.pallas import tpu as pltpu
from jax.sharding import PartitionSpec as P

GROUPS = 32
EPS = 1e-06
CHUNK = 128
MESH = pl.DeviceIdType.MESH
LOG2E = math.log2(math.e)
NT = (((1,), (1,)), ((), ()))


def exact_dot(vectors, matrix):
    index = lax.broadcasted_iota(jnp.int32, (16, vectors[0].shape[1]), 0)
    parts = jnp.zeros(index.shape, jnp.float32)
    for i, vector in enumerate(vectors):
        high = vector.astype(jnp.bfloat16).astype(jnp.float32)
        rest = vector - high
        mid = rest.astype(jnp.bfloat16).astype(jnp.float32)
        for j, part in enumerate((high, mid, rest - mid)):
            parts = jnp.where(index == 3 * i + j, part, parts)
    sums = jnp.dot(parts.astype(jnp.bfloat16), matrix, preferred_element_type=jnp.float32)
    return [
        sums[3 * i : 3 * i + 1] + sums[3 * i + 1 : 3 * i + 2] + sums[3 * i + 2 : 3 * i + 3]
        for i in range(len(vectors))
    ]


def kernel(
    n, wide,
    latent, w_query, w_key, w_value, w_out, w_conv,
    attn_gain_in, attn_shift_in, conv_gain_in, conv_shift_in, conv_bias_in,
    out,
    kv, wq, wk, wv, wo, wvo, wc, ones, fold, spread, moments, queries, bias, maxima, total, acc, hidden, halo, stacked,
    load_sem, weight_sem, send_sem, recv_sem, stat_send, stat_recv, halo_send, halo_recv,
    result, store_sem, vectors, vector_sem, entered,
):
    deep, chunks, _, chunk, channels = kv.shape
    rows = chunks * chunk
    far = deep // 2
    half_chunks = chunks // 2
    early = 2
    lines = rows // wide
    size = channels // GROUPS
    img = lax.axis_index("img")
    r = lax.axis_index("row")
    z = r // 2
    c = r % 2
    partner = r + 1 - 2 * c

    barrier = pltpu.get_barrier_semaphore()

    upward, downward = lax.rem(r + 2, n), lax.rem(r + n - 2, n)
    for target in (upward, downward, partner):
        pl.semaphore_signal(barrier, inc=1, device_id=(img, target), device_id_type=MESH)

    loads = [
        pltpu.make_async_copy(latent.at[k], kv.at[z, k, c], load_sem.at[k]) for k in range(chunks)
    ]
    for load in loads:
        load.start()
    weights = [
        pltpu.make_async_copy(source, target, weight_sem.at[i])
        for i, (source, target) in enumerate([(w_query, wq), (w_key, wk), (w_value, wv), (w_out, wo)])
    ]
    weights += [
        pltpu.make_async_copy(
            w_conv.at[dy, dx],
            wc.at[dx, pl.ds(dy * channels, channels)],
            weight_sem.at[4 + dy * 3 + dx],
        )
        for dy in range(3)
        for dx in range(3)
    ]
    for weight in weights:
        weight.start()

    small = [
        pltpu.make_async_copy(source, vectors.at[pl.ds(i, 1)], vector_sem.at[i])
        for i, source in enumerate(
            [attn_gain_in, attn_shift_in, conv_gain_in, conv_shift_in, conv_bias_in]
        )
    ]
    for copy in small:
        copy.start()

    def piece(way, zb, k):
        target = (upward, downward, partner)[way]
        return pltpu.make_async_remote_copy(
            src_ref=kv.at[zb, k, c],
            dst_ref=kv.at[zb, k, c],
            send_sem=send_sem.at[way, zb, k],
            recv_sem=recv_sem.at[c, zb, k],
            device_id=(img, target),
            device_id_type=MESH,
        )

    def arrival(core, zb, k):
        return pltpu.make_async_remote_copy(
            src_ref=kv.at[zb, k, core],
            dst_ref=kv.at[zb, k, core],
            send_sem=send_sem.at[0, 0, 0],
            recv_sem=recv_sem.at[core, zb, k],
            device_id=(img, partner),
            device_id_type=MESH,
        )

    def stat_copy(which, j):
        return pltpu.make_async_remote_copy(
            src_ref=moments.at[which, r],
            dst_ref=moments.at[which, r],
            send_sem=stat_send.at[which, j],
            recv_sem=stat_recv.at[which, r],
            device_id=(img, lax.rem(r + j, n)),
            device_id_type=MESH,
        )

    def stat_arrival(which, b):
        return pltpu.make_async_remote_copy(
            src_ref=moments.at[which, b],
            dst_ref=moments.at[which, b],
            send_sem=stat_send.at[which, 0],
            recv_sem=stat_recv.at[which, b],
            device_id=(img, partner),
            device_id_type=MESH,
        )

    def own():
        return kv[z, :, c]

    def send_own(k):
        piece(0, z, k).start()
        piece(1, z, k).start()
        piece(2, z, k).start()

    def split(way, d, k):
        part = (k < half_chunks) if way == 0 else (k >= half_chunks)
        return jnp.logical_or(d < far, jnp.logical_and(d == far, part))

    own_steps = half_chunks

    def spot(way, s):
        e = s - own_steps
        d = jnp.where(e < 0, 0, e // chunks + 1)
        last = d == far
        step = jnp.where(e < 0, 2 * s + way, lax.rem(e + chunks, chunks) + jnp.where(last, way * half_chunks, 0))
        zb = lax.rem(z + (deep - d if way == 0 else d), deep)
        return d, zb, step

    def relay(s):
        for way in (0, 1):
            d, zb, k = spot(way, s)
            arrival(c, zb, k).wait_recv()

            @pl.when(split(way, d + 1, k))
            def _(way=way, zb=zb, k=k):
                piece(way, zb, k).start()

            piece(2, zb, k).start()

    def share_moments(which, field):
        mean = jnp.sum(field, axis=0, keepdims=True) * (1.0 / rows)
        offset = field - mean
        square = jnp.sum(offset * offset, axis=0, keepdims=True)
        (near,) = exact_dot([mean], ones[...])
        away = mean - near * (1.0 / size)
        sums, squares = exact_dot([mean, square + rows * (away * away)], fold[...])
        moments[which, r, 0:1, :] = sums * (1.0 / size)
        moments[which, r, 1:2, :] = squares

        @pl.loop(1, n)
        def _(j):
            stat_copy(which, j).start()

    def gather_moments(which):
        @pl.loop(1, n)
        def _(j):
            stat_arrival(which, lax.rem(r + j, n)).wait_recv()

        @pl.loop(1, n)
        def _(j):
            stat_copy(which, j).wait_send()

        every = moments[which]
        means = every[:, 0, :]
        squares = every[:, 1, :]
        centre = jnp.sum(means, axis=0, keepdims=True) * (1.0 / n)
        away = means - centre
        whole = jnp.sum(squares + (rows * size) * (away * away), axis=0, keepdims=True)
        scale = lax.rsqrt(whole * (1.0 / (n * size * rows)) + EPS)
        return exact_dot([centre, scale], spread[...])

    def groups(shape, left, right):
        rows_of, columns_of = (lax.broadcasted_iota(jnp.int32, shape, i) for i in (0, 1))
        return jnp.where(rows_of // left == columns_of // right, 1.0, 0.0).astype(jnp.bfloat16)

    ones[...] = groups(ones.shape, size, size)
    fold[...] = groups(fold.shape, size, 1)
    spread[...] = groups(spread.shape, 1, size)
    maxima[...] = jnp.full_like(maxima, -1e30)
    total[...] = jnp.zeros_like(total)
    acc[...] = jnp.zeros_like(acc)

    pl.semaphore_wait(barrier, 3)
    for k in range(chunks):
        loads[k].wait()
        if k < early:
            send_own(k)
    for j in range(far - 1):
        for target in (upward, downward):
            pl.semaphore_signal(
                entered.at[j], inc=1, device_id=(img, target), device_id_type=MESH
            )
        pl.semaphore_wait(entered.at[j], 2)
    pl.semaphore_signal(entered.at[far - 1], inc=1, device_id=(img, partner), device_id_type=MESH)
    pl.semaphore_wait(entered.at[far - 1], 1)
    share_moments(0, own().reshape(rows, channels).astype(jnp.float32))
    for k in range(early, chunks):
        send_own(k)

    for s in (own_steps, own_steps + 1):
        relay(s)

    for weight in weights[:2]:
        weight.wait()
    for copy in small:
        copy.wait()
    attn_gain, attn_shift, conv_gain, conv_shift = (vectors[i : i + 1] for i in range(4))
    conv_bias = vectors.at[4:5]
    centre, scale = gather_moments(0)
    gain = scale * attn_gain
    positions = own().reshape(rows, channels).astype(jnp.float32)
    normed = ((positions - centre) * gain + attn_shift).astype(jnp.bfloat16)
    query = jnp.dot(normed, wq[...], preferred_element_type=jnp.float32).astype(jnp.bfloat16)
    folded = lax.dot_general(query, wk[...], NT, preferred_element_type=jnp.float32) * (
        LOG2E / math.sqrt(channels)
    )
    queries[...] = (folded * gain).astype(jnp.bfloat16)
    constant = jnp.sum(folded * (attn_shift - centre * gain), axis=1, keepdims=True)
    bias[...] = jnp.broadcast_to(constant, bias.shape)

    for weight in weights[2:4]:
        weight.wait()
    wvo[...] = jnp.dot(wv[...], wo[...], preferred_element_type=jnp.float32).astype(jnp.bfloat16)

    lanes = 128
    halves = [slice(i, i + rows // 2) for i in range(0, rows, rows // 2)]

    def attend(blocks):
        scores = [
            [
                lax.dot_general(queries[part], block, NT, preferred_element_type=jnp.float32)
                for block in blocks
            ]
            for part in halves
        ]
        for part, pair in zip(halves, scores):
            columns = [
                score[:, j : j + lanes] for score in pair for j in range(0, 2 * chunk, lanes)
            ]
            peak = functools.reduce(jnp.maximum, columns)
            offset = bias[part]
            newest = jnp.maximum(maxima[part], jnp.max(peak, axis=1, keepdims=True) + offset)
            fade = jnp.exp2(maxima[part] - newest)
            maxima[part] = newest
            level = newest - offset
            weights = [jnp.exp2(column - level) for column in columns]
            total[part] = functools.reduce(jnp.add, weights, total[part] * fade)
            each = len(weights) // len(blocks)
            product = 0.0
            for i, block in enumerate(blocks):
                probs = jnp.concatenate(weights[i * each : (i + 1) * each], axis=1)
                product = product + jnp.dot(
                    probs.astype(jnp.bfloat16), block, preferred_element_type=jnp.float32
                )
            acc[part] = acc[part] * jnp.tile(fade, (1, channels // lanes)) + product

    relay(own_steps + 2)
    steps = own_steps + (far - 1) * chunks + half_chunks
    lead = 2
    taper = 6

    @pl.loop(0, steps - 1)
    def _(s):
        @pl.when(jnp.logical_and(s >= 3, s < taper))
        def _():
            relay(s + lead)

        @pl.when(s >= taper + lead)
        def _():
            relay(s)

        blocks = []
        for way in (0, 1):
            d, zb, k = spot(way, s)
            arrival(1 - c, zb, k).wait_recv()
            blocks.append(kv[zb, k].reshape(2 * chunk, channels))
        attend(blocks)

    final = [spot(way, steps - 1) for way in (0, 1)]
    relay(steps - 1)
    attend([jnp.concatenate([kv[zb, k, c] for d, zb, k in final], axis=0)])
    for d, zb, k in final:
        arrival(1 - c, zb, k).wait_recv()
    attend([jnp.concatenate([kv[zb, k, 1 - c] for d, zb, k in final], axis=0)])

    denominator = jnp.sum(total[...], axis=1, keepdims=True)
    average = (acc[...] * (1.0 / denominator) - centre) * gain + attn_shift
    attended = jnp.dot(
        average.astype(jnp.bfloat16), wvo[...], preferred_element_type=jnp.float32
    )
    field = (own().reshape(rows, channels).astype(jnp.float32) + attended).astype(jnp.bfloat16)
    hidden[...] = field
    share_moments(1, field.astype(jnp.float32))

    up = pltpu.make_async_remote_copy(
        src_ref=hidden.at[pl.ds(0, wide)],
        dst_ref=halo.at[1],
        send_sem=halo_send.at[1],
        recv_sem=halo_recv.at[1],
        device_id=(img, r - 1),
        device_id_type=MESH,
    )
    down = pltpu.make_async_remote_copy(
        src_ref=hidden.at[pl.ds(rows - wide, wide)],
        dst_ref=halo.at[0],
        send_sem=halo_send.at[0],
        recv_sem=halo_recv.at[0],
        device_id=(img, r + 1),
        device_id_type=MESH,
    )

    @pl.when(r > 0)
    def _():
        up.start()

    @pl.when(r < n - 1)
    def _():
        down.start()

    @pl.loop(0, deep * chunks)
    def _(t):
        zb = t // chunks
        k = t % chunks

        @pl.when(split(0, lax.rem(z + deep - zb, deep) + 1, k))
        def _():
            piece(0, zb, k).wait_send()

        @pl.when(split(1, lax.rem(zb + deep - z, deep) + 1, k))
        def _():
            piece(1, zb, k).wait_send()

        piece(2, zb, k).wait_send()

    for weight in weights[4:]:
        weight.wait()
    centre, scale = gather_moments(1)
    gain = scale * conv_gain

    def activate(values):
        v = (values.astype(jnp.float32) - centre) * gain + conv_shift
        return (v / (1.0 + jnp.exp(-v))).astype(jnp.bfloat16)

    order = [*range(1, lines - 1), 0, lines - 1]

    def place(line, values):
        for dy in range(3):
            y = line + 1 - dy
            if 0 <= y < lines:
                slot = order.index(y) * wide
                stacked[slot : slot + wide, dy * channels : (dy + 1) * channels] = values

    def convolve(first, last):
        count = (last - first) * wide
        window = stacked[first * wide : last * wide]
        column = lax.broadcasted_iota(jnp.int32, (count, channels), 0) % wide

        def taps(dx):
            return jnp.dot(window, wc[dx], preferred_element_type=jnp.float32)

        convolved = taps(1) + conv_bias[...]
        convolved = convolved + jnp.where(column > 0, pltpu.roll(taps(0), 1, 0), 0.0)
        convolved = convolved + jnp.where(
            column < wide - 1, pltpu.roll(taps(2), count - 1, 0), 0.0
        )
        stores = []
        for i, y in enumerate(order[first:last]):
            line = slice(y * wide, (y + 1) * wide)
            part = convolved[i * wide : (i + 1) * wide]
            result[line] = (hidden[line].astype(jnp.float32) + part).astype(jnp.bfloat16)
            store = pltpu.make_async_copy(result.at[line], out.at[line], store_sem.at[y])
            store.start()
            stores.append(store)
        return stores

    for line in range(lines):
        place(line, activate(hidden[line * wide : (line + 1) * wide]))
    stores = convolve(0, lines - 2)

    @pl.when(r > 0)
    def _():
        up.wait_send()
        down.wait_recv()
        place(-1, activate(halo[0]))

    @pl.when(r == 0)
    def _():
        place(-1, jnp.zeros((wide, channels), jnp.bfloat16))

    @pl.when(r < n - 1)
    def _():
        down.wait_send()
        up.wait_recv()
        place(lines, activate(halo[1]))

    @pl.when(r == n - 1)
    def _():
        place(lines, jnp.zeros((wide, channels), jnp.bfloat16))

    stores += convolve(lines - 2, lines)
    for store in stores:
        store.wait()


def local(n, latent, attn_gain, attn_shift, w_query, w_key, w_value, w_out,
          conv_gain, conv_shift, w_conv, conv_bias):
    height, wide, channels = latent.shape
    rows = height * wide
    chunks = rows // CHUNK
    anywhere = pl.BlockSpec(memory_space=pl.ANY)
    bf16, f32 = jnp.bfloat16, jnp.float32
    square = pltpu.VMEM((channels, channels), bf16)
    dma = pltpu.SemaphoreType.DMA
    encoded = pl.pallas_call(
        functools.partial(kernel, n, wide),
        out_shape=jax.ShapeDtypeStruct((rows, channels), bf16),
        in_specs=[anywhere] * 11,
        out_specs=anywhere,
        scratch_shapes=[
            pltpu.VMEM((n // 2, chunks, 2, CHUNK, channels), bf16),
            square, square, square, square, square,
            pltpu.VMEM((3, 3 * channels, channels), bf16),
            square,
            pltpu.VMEM((channels, 128), bf16),
            pltpu.VMEM((128, channels), bf16),
            pltpu.VMEM((2, n, 2, 128), f32),
            pltpu.VMEM((rows, channels), bf16),
            pltpu.VMEM((rows, 128), f32),
            pltpu.VMEM((rows, 128), f32),
            pltpu.VMEM((rows, 128), f32),
            pltpu.VMEM((rows, channels), f32),
            pltpu.VMEM((rows, channels), bf16),
            pltpu.VMEM((2, wide, channels), bf16),
            pltpu.VMEM((rows, 3 * channels), bf16),
            dma((chunks,)),
            dma((13,)),
            dma((3, n // 2, chunks)),
            dma((2, n // 2, chunks)),
            dma((2, n)),
            dma((2, n)),
            dma((2,)),
            dma((2,)),
            pltpu.VMEM((rows, channels), bf16),
            dma((height,)),
            pltpu.VMEM((8, channels), f32),
            dma((5,)),
            pltpu.SemaphoreType.REGULAR((n // 4,)),
        ],
        compiler_params=pltpu.CompilerParams(
            collective_id=0, has_side_effects=True, vmem_limit_bytes=56 * 1024 * 1024
        ),
    )(
        latent.reshape(chunks, CHUNK, channels), w_query, w_key, w_value, w_out, w_conv,
        *(v.reshape(1, channels) for v in (attn_gain, attn_shift, conv_gain, conv_shift, conv_bias)),
    )
    return encoded.reshape(height, wide, channels)


def solution(mesh):
    in_specs = (P(("img", "row"), None, None), P(), P(), P(), P(), P(), P(), P(), P(), P(), P())
    out_specs = P(("img", "row"), None, None)
    body = functools.partial(local, mesh.shape["row"])
    return jax.shard_map(body, mesh=mesh, in_specs=in_specs, out_specs=out_specs, check_vma=False)
```

```python
import functools
import math

import jax
import jax.numpy as jnp
from jax import lax
from jax.experimental import pallas as pl
from jax.experimental.pallas import tpu as pltpu
from jax.sharding import PartitionSpec as P

GROUPS = 32
EPS = 1e-06
CHUNK = 128
MESH = pl.DeviceIdType.MESH
LOG2E = math.log2(math.e)
NT = (((1,), (1,)), ((), ()))


def exact_dot(vectors, matrix):
    index = lax.broadcasted_iota(jnp.int32, (16, vectors[0].shape[1]), 0)
    parts = jnp.zeros(index.shape, jnp.float32)
    for i, vector in enumerate(vectors):
        high = vector.astype(jnp.bfloat16).astype(jnp.float32)
        rest = vector - high
        mid = rest.astype(jnp.bfloat16).astype(jnp.float32)
        for j, part in enumerate((high, mid, rest - mid)):
            parts = jnp.where(index == 3 * i + j, part, parts)
    sums = jnp.dot(parts.astype(jnp.bfloat16), matrix, preferred_element_type=jnp.float32)
    return [
        sums[3 * i : 3 * i + 1] + sums[3 * i + 1 : 3 * i + 2] + sums[3 * i + 2 : 3 * i + 3]
        for i in range(len(vectors))
    ]


def kernel(
    n, wide,
    latent, w_query, w_key, w_value, w_out, w_conv,
    attn_gain_in, attn_shift_in, conv_gain_in, conv_shift_in, conv_bias_in,
    out,
    kv, wq, wk, wv, wo, wvo, wc, ones, fold, spread, moments, queries, bias, maxima, total, acc, hidden, halo, stacked,
    load_sem, weight_sem, send_sem, recv_sem, stat_send, stat_recv, halo_send, halo_recv,
    vectors, vector_sem, entered,
):
    deep, chunks, _, chunk, channels = kv.shape
    rows = chunks * chunk
    far = deep // 2
    half_chunks = chunks // 2
    early = 3
    primed = 3
    lead = 3
    lines = rows // wide
    size = channels // GROUPS
    img = lax.axis_index("img")
    r = lax.axis_index("row")
    z = r // 2
    c = r % 2
    partner = r + 1 - 2 * c

    barrier = pltpu.get_barrier_semaphore()

    upward, downward = lax.rem(r + 2, n), lax.rem(r + n - 2, n)
    for target in (upward, downward, partner):
        pl.semaphore_signal(barrier, inc=1, device_id=(img, target), device_id_type=MESH)

    loads = [
        pltpu.make_async_copy(latent.at[k], kv.at[z, k, c], load_sem.at[k]) for k in range(chunks)
    ]
    for load in loads:
        load.start()
    weights = [
        pltpu.make_async_copy(source, target, weight_sem.at[i])
        for i, (source, target) in enumerate([(w_query, wq), (w_key, wk), (w_value, wv), (w_out, wo)])
    ]
    weights += [
        pltpu.make_async_copy(
            w_conv.at[dy, dx],
            wc.at[dx, pl.ds(dy * channels, channels)],
            weight_sem.at[4 + dy * 3 + dx],
        )
        for dy in range(3)
        for dx in range(3)
    ]
    for weight in weights:
        weight.start()

    small = [
        pltpu.make_async_copy(source, vectors.at[pl.ds(i, 1)], vector_sem.at[i])
        for i, source in enumerate(
            [attn_gain_in, attn_shift_in, conv_gain_in, conv_shift_in, conv_bias_in]
        )
    ]
    for copy in small:
        copy.start()

    def piece(way, zb, k):
        target = (upward, downward, partner)[way]
        return pltpu.make_async_remote_copy(
            src_ref=kv.at[zb, k, c],
            dst_ref=kv.at[zb, k, c],
            send_sem=send_sem.at[way, zb, k],
            recv_sem=recv_sem.at[c, zb, k],
            device_id=(img, target),
            device_id_type=MESH,
        )

    def arrival(core, zb, k):
        return pltpu.make_async_remote_copy(
            src_ref=kv.at[zb, k, core],
            dst_ref=kv.at[zb, k, core],
            send_sem=send_sem.at[0, 0, 0],
            recv_sem=recv_sem.at[core, zb, k],
            device_id=(img, partner),
            device_id_type=MESH,
        )

    def stat_copy(which, j):
        return pltpu.make_async_remote_copy(
            src_ref=moments.at[which, r],
            dst_ref=moments.at[which, r],
            send_sem=stat_send.at[which, j],
            recv_sem=stat_recv.at[which, r],
            device_id=(img, lax.rem(r + j, n)),
            device_id_type=MESH,
        )

    def stat_arrival(which, b):
        return pltpu.make_async_remote_copy(
            src_ref=moments.at[which, b],
            dst_ref=moments.at[which, b],
            send_sem=stat_send.at[which, 0],
            recv_sem=stat_recv.at[which, b],
            device_id=(img, partner),
            device_id_type=MESH,
        )

    def own():
        return kv[z, :, c]

    def send_own(k):
        piece(0, z, k).start()
        piece(1, z, k).start()
        piece(2, z, k).start()

    def split(way, d, k):
        part = (k < half_chunks) if way == 0 else (k >= half_chunks)
        return jnp.logical_or(d < far, jnp.logical_and(d == far, part))

    own_steps = half_chunks

    def spot(way, s):
        e = s - own_steps
        d = jnp.where(e < 0, 0, e // chunks + 1)
        last = d == far
        step = jnp.where(e < 0, 2 * s + way, lax.rem(e + chunks, chunks) + jnp.where(last, way * half_chunks, 0))
        zb = lax.rem(z + (deep - d if way == 0 else d), deep)
        return d, zb, step

    def relay(s):
        for way in (0, 1):
            d, zb, k = spot(way, s)
            arrival(c, zb, k).wait_recv()

            @pl.when(split(way, d + 1, k))
            def _(way=way, zb=zb, k=k):
                piece(way, zb, k).start()

            piece(2, zb, k).start()

    def share_moments(which, field):
        mean = jnp.sum(field, axis=0, keepdims=True) * (1.0 / rows)
        offset = field - mean
        square = jnp.sum(offset * offset, axis=0, keepdims=True)
        (near,) = exact_dot([mean], ones[...])
        away = mean - near * (1.0 / size)
        sums, squares = exact_dot([mean, square + rows * (away * away)], fold[...])
        moments[which, r, 0:1, :] = sums * (1.0 / size)
        moments[which, r, 1:2, :] = squares

        @pl.loop(1, n)
        def _(j):
            stat_copy(which, j).start()

    def gather_moments(which):
        @pl.loop(1, n)
        def _(j):
            stat_arrival(which, lax.rem(r + j, n)).wait_recv()

        every = moments[which]
        means = every[:, 0, :]
        squares = every[:, 1, :]
        centre = jnp.sum(means, axis=0, keepdims=True) * (1.0 / n)
        away = means - centre
        whole = jnp.sum(squares + (rows * size) * (away * away), axis=0, keepdims=True)
        scale = lax.rsqrt(whole * (1.0 / (n * size * rows)) + EPS)
        return exact_dot([centre, scale], spread[...])

    pl.semaphore_wait(barrier, 3)
    for k in range(chunks):
        loads[k].wait()
        if k < early:
            send_own(k)
    def groups(shape, left, right):
        rows_of, columns_of = (lax.broadcasted_iota(jnp.int32, shape, i) for i in (0, 1))
        return jnp.where(rows_of // left == columns_of // right, 1.0, 0.0).astype(jnp.bfloat16)

    def prepare(j):
        if j == 0:
            ones[...] = groups(ones.shape, size, size)
        if j == 1:
            fold[...] = groups(fold.shape, size, 1)
            spread[...] = groups(spread.shape, 1, size)
            maxima[...] = jnp.full_like(maxima, -1e30)
            total[...] = jnp.zeros_like(total)
        if j == 2:
            acc[...] = jnp.zeros_like(acc)

    for j in range(far - 1):
        for target in (upward, downward):
            pl.semaphore_signal(
                entered.at[j], inc=1, device_id=(img, target), device_id_type=MESH
            )
        prepare(j)
        pl.semaphore_wait(entered.at[j], 2)
    pl.semaphore_signal(entered.at[far - 1], inc=1, device_id=(img, partner), device_id_type=MESH)
    pl.semaphore_wait(entered.at[far - 1], 1)
    share_moments(0, own().reshape(rows, channels).astype(jnp.float32))
    for k in range(early, chunks):
        send_own(k)

    for s in range(own_steps, own_steps + primed):
        relay(s)

    for weight in weights[:2]:
        weight.wait()
    for copy in small:
        copy.wait()
    attn_gain, attn_shift, conv_gain, conv_shift = (vectors[i : i + 1] for i in range(4))
    conv_bias = vectors.at[4:5]
    centre, scale = gather_moments(0)
    gain = scale * attn_gain
    positions = own().reshape(rows, channels).astype(jnp.float32)
    normed = ((positions - centre) * gain + attn_shift).astype(jnp.bfloat16)
    query = jnp.dot(normed, wq[...], preferred_element_type=jnp.float32).astype(jnp.bfloat16)
    folded = lax.dot_general(query, wk[...], NT, preferred_element_type=jnp.float32) * (
        LOG2E / math.sqrt(channels)
    )
    queries[...] = (folded * gain).astype(jnp.bfloat16)
    constant = jnp.sum(folded * (attn_shift - centre * gain), axis=1, keepdims=True)
    bias[...] = jnp.broadcast_to(constant, bias.shape)

    for weight in weights[2:4]:
        weight.wait()
    wvo[...] = jnp.dot(wv[...], wo[...], preferred_element_type=jnp.float32).astype(jnp.bfloat16)

    lanes = 128
    halves = [slice(i, i + rows // 2) for i in range(0, rows, rows // 2)]

    def attend(blocks):
        scores = [
            [
                lax.dot_general(queries[part], block, NT, preferred_element_type=jnp.float32)
                for block in blocks
            ]
            for part in halves
        ]
        for part, pair in zip(halves, scores):
            columns = [
                score[:, j : j + lanes] for score in pair for j in range(0, 2 * chunk, lanes)
            ]
            peak = functools.reduce(jnp.maximum, columns)
            offset = bias[part]
            newest = jnp.maximum(maxima[part], jnp.max(peak, axis=1, keepdims=True) + offset)
            fade = jnp.exp2(maxima[part] - newest)
            maxima[part] = newest
            level = newest - offset
            weights = [jnp.exp2(column - level) for column in columns]
            total[part] = functools.reduce(jnp.add, weights, total[part] * fade)
            each = len(weights) // len(blocks)
            product = 0.0
            for i, block in enumerate(blocks):
                probs = jnp.concatenate(weights[i * each : (i + 1) * each], axis=1)
                product = product + jnp.dot(
                    probs.astype(jnp.bfloat16), block, preferred_element_type=jnp.float32
                )
            acc[part] = acc[part] * jnp.tile(fade, (1, channels // lanes)) + product

    steps = own_steps + (far - 1) * chunks + half_chunks
    first = own_steps + primed - lead
    taper = first + 3

    @pl.loop(0, steps - 1)
    def _(s):
        @pl.when(jnp.logical_and(s >= first, s < taper))
        def _():
            relay(s + lead)

        @pl.when(s >= taper + lead)
        def _():
            relay(s)

        blocks = []
        for way in (0, 1):
            d, zb, k = spot(way, s)
            arrival(1 - c, zb, k).wait_recv()
            blocks.append(kv[zb, k].reshape(2 * chunk, channels))
        attend(blocks)

    final = [spot(way, steps - 1) for way in (0, 1)]
    relay(steps - 1)
    attend([jnp.concatenate([kv[zb, k, c] for d, zb, k in final], axis=0)])
    for d, zb, k in final:
        arrival(1 - c, zb, k).wait_recv()
    attend([jnp.concatenate([kv[zb, k, 1 - c] for d, zb, k in final], axis=0)])

    denominator = jnp.sum(total[...], axis=1, keepdims=True)
    average = (acc[...] * (1.0 / denominator) - centre) * gain + attn_shift
    attended = jnp.dot(
        average.astype(jnp.bfloat16), wvo[...], preferred_element_type=jnp.float32
    )
    field = (own().reshape(rows, channels).astype(jnp.float32) + attended).astype(jnp.bfloat16)
    hidden[...] = field
    share_moments(1, field.astype(jnp.float32))

    up = pltpu.make_async_remote_copy(
        src_ref=hidden.at[pl.ds(0, wide)],
        dst_ref=halo.at[1],
        send_sem=halo_send.at[1],
        recv_sem=halo_recv.at[1],
        device_id=(img, r - 1),
        device_id_type=MESH,
    )
    down = pltpu.make_async_remote_copy(
        src_ref=hidden.at[pl.ds(rows - wide, wide)],
        dst_ref=halo.at[0],
        send_sem=halo_send.at[0],
        recv_sem=halo_recv.at[0],
        device_id=(img, r + 1),
        device_id_type=MESH,
    )

    @pl.when(r > 0)
    def _():
        up.start()

    @pl.when(r < n - 1)
    def _():
        down.start()

    @pl.loop(0, deep * chunks)
    def _(t):
        zb = t // chunks
        k = t % chunks

        @pl.when(split(0, lax.rem(z + deep - zb, deep) + 1, k))
        def _():
            piece(0, zb, k).wait_send()

        @pl.when(split(1, lax.rem(zb + deep - z, deep) + 1, k))
        def _():
            piece(1, zb, k).wait_send()

        piece(2, zb, k).wait_send()

    for weight in weights[4:]:
        weight.wait()
    centre, scale = gather_moments(1)
    gain = scale * conv_gain

    def activate(values):
        v = (values.astype(jnp.float32) - centre) * gain + conv_shift
        return (v / (1.0 + jnp.exp(-v))).astype(jnp.bfloat16)

    order = [*range(1, lines - 1), 0, lines - 1]

    def place(line, values):
        for dy in range(3):
            y = line + 1 - dy
            if 0 <= y < lines:
                slot = order.index(y) * wide
                stacked[slot : slot + wide, dy * channels : (dy + 1) * channels] = values

    def convolve(first, last):
        count = (last - first) * wide
        window = stacked[first * wide : last * wide]
        column = lax.broadcasted_iota(jnp.int32, (count, channels), 0) % wide

        def taps(dx):
            return jnp.dot(window, wc[dx], preferred_element_type=jnp.float32)

        convolved = taps(1) + conv_bias[...]
        convolved = convolved + jnp.where(column > 0, pltpu.roll(taps(0), 1, 0), 0.0)
        convolved = convolved + jnp.where(
            column < wide - 1, pltpu.roll(taps(2), count - 1, 0), 0.0
        )
        for i, y in enumerate(order[first:last]):
            line = slice(y * wide, (y + 1) * wide)
            part = convolved[i * wide : (i + 1) * wide]
            out[line] = (hidden[line].astype(jnp.float32) + part).astype(jnp.bfloat16)

    for line in range(lines):
        place(line, activate(hidden[line * wide : (line + 1) * wide]))
    convolve(0, lines - 2)

    @pl.when(r > 0)
    def _():
        up.wait_send()
        down.wait_recv()
        place(-1, activate(halo[0]))

    @pl.when(r == 0)
    def _():
        place(-1, jnp.zeros((wide, channels), jnp.bfloat16))

    @pl.when(r < n - 1)
    def _():
        down.wait_send()
        up.wait_recv()
        place(lines, activate(halo[1]))

    @pl.when(r == n - 1)
    def _():
        place(lines, jnp.zeros((wide, channels), jnp.bfloat16))

    convolve(lines - 2, lines)

    for which in range(2):
        @pl.loop(1, n)
        def _(j, which=which):
            stat_copy(which, j).wait_send()


def local(n, latent, attn_gain, attn_shift, w_query, w_key, w_value, w_out,
          conv_gain, conv_shift, w_conv, conv_bias):
    height, wide, channels = latent.shape
    rows = height * wide
    chunks = rows // CHUNK
    anywhere = pl.BlockSpec(memory_space=pl.ANY)
    bf16, f32 = jnp.bfloat16, jnp.float32
    square = pltpu.VMEM((channels, channels), bf16)
    dma = pltpu.SemaphoreType.DMA
    def kept(value):
        return pltpu.with_memory_space_constraint(value, pltpu.HBM)

    encoded = pl.pallas_call(
        functools.partial(kernel, n, wide),
        out_shape=jax.ShapeDtypeStruct((rows, channels), bf16),
        in_specs=[anywhere] * 11,
        out_specs=pl.BlockSpec(memory_space=pltpu.VMEM),
        scratch_shapes=[
            pltpu.VMEM((n // 2, chunks, 2, CHUNK, channels), bf16),
            square, square, square, square, square,
            pltpu.VMEM((3, 3 * channels, channels), bf16),
            square,
            pltpu.VMEM((channels, 128), bf16),
            pltpu.VMEM((128, channels), bf16),
            pltpu.VMEM((2, n, 2, 128), f32),
            pltpu.VMEM((rows, channels), bf16),
            pltpu.VMEM((rows, 128), f32),
            pltpu.VMEM((rows, 128), f32),
            pltpu.VMEM((rows, 128), f32),
            pltpu.VMEM((rows, channels), f32),
            pltpu.VMEM((rows, channels), bf16),
            pltpu.VMEM((2, wide, channels), bf16),
            pltpu.VMEM((rows, 3 * channels), bf16),
            dma((chunks,)),
            dma((13,)),
            dma((3, n // 2, chunks)),
            dma((2, n // 2, chunks)),
            dma((2, n)),
            dma((2, n)),
            dma((2,)),
            dma((2,)),
            pltpu.VMEM((8, channels), f32),
            dma((5,)),
            pltpu.SemaphoreType.REGULAR((n // 4,)),
        ],
        compiler_params=pltpu.CompilerParams(
            collective_id=0, has_side_effects=True, vmem_limit_bytes=48 * 1024 * 1024
        ),
    )(
        *map(kept, (latent.reshape(chunks, CHUNK, channels), w_query, w_key, w_value, w_out, w_conv)),
        *(kept(v.reshape(1, channels)) for v in (attn_gain, attn_shift, conv_gain, conv_shift, conv_bias)),
    )
    return encoded.reshape(height, wide, channels)


def solution(mesh):
    in_specs = (P(("img", "row"), None, None), P(), P(), P(), P(), P(), P(), P(), P(), P(), P())
    out_specs = P(("img", "row"), None, None)
    body = functools.partial(local, mesh.shape["row"])
    return jax.shard_map(body, mesh=mesh, in_specs=in_specs, out_specs=out_specs, check_vma=False)
```

```python
import functools
import math

import jax
import jax.numpy as jnp
from jax import lax
from jax.experimental import pallas as pl
from jax.experimental.pallas import tpu as pltpu
from jax.sharding import PartitionSpec as P

GROUPS = 32
EPS = 1e-06
CHUNK = 128
MESH = pl.DeviceIdType.MESH
LOG2E = math.log2(math.e)
NT = (((1,), (1,)), ((), ()))


def exact_dot(vectors, matrix):
    index = lax.broadcasted_iota(jnp.int32, (16, vectors[0].shape[1]), 0)
    parts = jnp.zeros(index.shape, jnp.float32)
    for i, vector in enumerate(vectors):
        high = vector.astype(jnp.bfloat16).astype(jnp.float32)
        rest = vector - high
        mid = rest.astype(jnp.bfloat16).astype(jnp.float32)
        for j, part in enumerate((high, mid, rest - mid)):
            parts = jnp.where(index == 3 * i + j, part, parts)
    sums = jnp.dot(parts.astype(jnp.bfloat16), matrix, preferred_element_type=jnp.float32)
    return [
        sums[3 * i : 3 * i + 1] + sums[3 * i + 1 : 3 * i + 2] + sums[3 * i + 2 : 3 * i + 3]
        for i in range(len(vectors))
    ]


def kernel(
    n, wide,
    latent, w_query, w_key, w_value, w_out, w_conv,
    attn_gain_in, attn_shift_in, conv_gain_in, conv_shift_in, conv_bias_in,
    out,
    kv, mats, wvo, wc, ones, fold, spread, moments, queries, bias, maxima, total, acc, hidden, halo, stacked,
    load_sem, weight_sem, send_sem, recv_sem, stat_send, stat_recv, halo_send, halo_recv,
    vectors, vector_sem, entered,
):
    deep, chunks, _, chunk, channels = kv.shape
    rows = chunks * chunk
    far = deep // 2
    half_chunks = chunks // 2
    own_steps = half_chunks
    early = 3
    primed = 3
    lead = 3
    lines = rows // wide
    size = channels // GROUPS
    img = lax.axis_index("img")
    r = lax.axis_index("row")
    z = r // 2
    c = r % 2
    partner = r + 1 - 2 * c

    barrier = pltpu.get_barrier_semaphore()

    upward, downward = lax.rem(r + 2, n), lax.rem(r + n - 2, n)
    for target in (upward, downward, partner):
        pl.semaphore_signal(barrier, inc=1, device_id=(img, target), device_id_type=MESH)

    loads = [
        pltpu.make_async_copy(latent.at[k], kv.at[z, k, c], load_sem.at[k]) for k in range(chunks)
    ]
    for load in loads:
        load.start()
    def filled(view, sem):
        pltpu.make_async_copy(view, view, sem).wait()

    for i, source in enumerate((w_query, w_key, w_value, w_out)):
        pltpu.make_async_copy(source, mats.at[i], weight_sem.at[i // 2]).start()
    for dy in range(3):
        for dx in range(3):
            pltpu.make_async_copy(
                w_conv.at[dy, dx], wc.at[dx, pl.ds(dy * channels, channels)], weight_sem.at[2]
            ).start()
    for i, source in enumerate(
        (attn_gain_in, attn_shift_in, conv_gain_in, conv_shift_in, conv_bias_in)
    ):
        pltpu.make_async_copy(source, vectors.at[i], vector_sem).start()

    def piece(way, zb, k, mark):
        return pltpu.make_async_remote_copy(
            src_ref=kv.at[zb, k, c],
            dst_ref=kv.at[zb, k, c],
            send_sem=send_sem.at[way],
            recv_sem=recv_sem.at[way // 2, mark],
            device_id=(img, (upward, downward, partner)[way]),
            device_id_type=MESH,
        )

    def whole(view, send, recv):
        return pltpu.make_async_remote_copy(
            src_ref=view,
            dst_ref=view,
            send_sem=send,
            recv_sem=recv,
            device_id=(img, partner),
            device_id_type=MESH,
        )

    def arrived(relayed, s):
        pair = kv.at[0, 0]
        whole(pair, send_sem.at[0], recv_sem.at[relayed, s]).wait_recv()

    def stat_copy(which, j):
        return pltpu.make_async_remote_copy(
            src_ref=moments.at[which, r],
            dst_ref=moments.at[which, r],
            send_sem=stat_send.at[which],
            recv_sem=stat_recv.at[which],
            device_id=(img, lax.rem(r + j, n)),
            device_id_type=MESH,
        )

    def stat_all(which):
        view = moments.at[which, pl.ds(0, n - 1)]
        return whole(view, stat_send.at[which], stat_recv.at[which])

    def own():
        return kv[z, :, c]

    def send_own(k):
        piece(0, z, k, own_steps + k).start()
        piece(1, z, k, own_steps + k).start()
        piece(2, z, k, k // 2).start()

    def split(way, d, k):
        part = (k < half_chunks) if way == 0 else (k >= half_chunks)
        return jnp.logical_or(d < far, jnp.logical_and(d == far, part))

    def spot(way, s):
        e = s - own_steps
        d = jnp.where(e < 0, 0, e // chunks + 1)
        last = d == far
        step = jnp.where(e < 0, 2 * s + way, lax.rem(e + chunks, chunks) + jnp.where(last, way * half_chunks, 0))
        zb = lax.rem(z + (deep - d if way == 0 else d), deep)
        return d, zb, step

    def relay(s):
        arrived(0, s)
        for way in (0, 1):
            d, zb, k = spot(way, s)
            mark = s + chunks - jnp.where(d + 1 == far, way * half_chunks, 0)

            @pl.when(split(way, d + 1, k))
            def _(way=way, zb=zb, k=k, mark=mark):
                piece(way, zb, k, mark).start()

            piece(2, zb, k, s).start()

    def share_moments(which, field):
        mean = jnp.sum(field, axis=0, keepdims=True) * (1.0 / rows)
        offset = field - mean
        square = jnp.sum(offset * offset, axis=0, keepdims=True)
        (near,) = exact_dot([mean], ones[...])
        away = mean - near * (1.0 / size)
        sums, squares = exact_dot([mean, square + rows * (away * away)], fold[...])
        moments[which, r, 0:1, :] = sums * (1.0 / size)
        moments[which, r, 1:2, :] = squares

        @pl.loop(1, n)
        def _(j):
            stat_copy(which, j).start()

    def gather_moments(which):
        stat_all(which).wait_recv()
        every = moments[which]
        means = every[:, 0, :]
        squares = every[:, 1, :]
        centre = jnp.sum(means, axis=0, keepdims=True) * (1.0 / n)
        away = means - centre
        whole = jnp.sum(squares + (rows * size) * (away * away), axis=0, keepdims=True)
        scale = lax.rsqrt(whole * (1.0 / (n * size * rows)) + EPS)
        return exact_dot([centre, scale], spread[...])

    pl.semaphore_wait(barrier, 3)
    for k in range(chunks):
        loads[k].wait()
        if k < early:
            send_own(k)
    def groups(shape, left, right):
        rows_of, columns_of = (lax.broadcasted_iota(jnp.int32, shape, i) for i in (0, 1))
        return jnp.where(rows_of // left == columns_of // right, 1.0, 0.0).astype(jnp.bfloat16)

    def prepare(j):
        if j == 0:
            ones[...] = groups(ones.shape, size, size)
        if j == 1:
            fold[...] = groups(fold.shape, size, 1)
            spread[...] = groups(spread.shape, 1, size)
            maxima[...] = jnp.full_like(maxima, -1e30)
            total[...] = jnp.zeros_like(total)
        if j == 2:
            acc[...] = jnp.zeros_like(acc)

    for j in range(far - 1):
        for target in (upward, downward):
            pl.semaphore_signal(
                entered.at[j], inc=1, device_id=(img, target), device_id_type=MESH
            )
        prepare(j)
        pl.semaphore_wait(entered.at[j], 2)
    pl.semaphore_signal(entered.at[far - 1], inc=1, device_id=(img, partner), device_id_type=MESH)
    pl.semaphore_wait(entered.at[far - 1], 1)
    share_moments(0, own().reshape(rows, channels).astype(jnp.float32))
    for k in range(early, chunks):
        send_own(k)

    for s in range(own_steps, own_steps + primed):
        relay(s)

    filled(mats.at[pl.ds(0, 2)], weight_sem.at[0])
    filled(vectors, vector_sem)
    attn_gain, attn_shift, conv_gain, conv_shift = (vectors[i] for i in range(4))
    conv_bias = vectors[4]
    centre, scale = gather_moments(0)
    gain = scale * attn_gain
    positions = own().reshape(rows, channels).astype(jnp.float32)
    normed = ((positions - centre) * gain + attn_shift).astype(jnp.bfloat16)
    query = jnp.dot(normed, mats[0], preferred_element_type=jnp.float32).astype(jnp.bfloat16)
    folded = lax.dot_general(query, mats[1], NT, preferred_element_type=jnp.float32) * (
        LOG2E / math.sqrt(channels)
    )
    queries[...] = (folded * gain).astype(jnp.bfloat16)
    constant = jnp.sum(folded * (attn_shift - centre * gain), axis=1, keepdims=True)
    bias[...] = jnp.broadcast_to(constant, bias.shape)

    filled(mats.at[pl.ds(2, 2)], weight_sem.at[1])
    wvo[...] = jnp.dot(mats[2], mats[3], preferred_element_type=jnp.float32).astype(jnp.bfloat16)

    lanes = 128
    halves = [slice(i, i + rows // 2) for i in range(0, rows, rows // 2)]

    def attend(blocks):
        scores = [
            [
                lax.dot_general(queries[part], block, NT, preferred_element_type=jnp.float32)
                for block in blocks
            ]
            for part in halves
        ]
        for part, pair in zip(halves, scores):
            columns = [
                score[:, j : j + lanes] for score in pair for j in range(0, 2 * chunk, lanes)
            ]
            peak = functools.reduce(jnp.maximum, columns)
            offset = bias[part]
            newest = jnp.maximum(maxima[part], jnp.max(peak, axis=1, keepdims=True) + offset)
            fade = jnp.exp2(maxima[part] - newest)
            maxima[part] = newest
            level = newest - offset
            weights = [jnp.exp2(column - level) for column in columns]
            total[part] = functools.reduce(jnp.add, weights, total[part] * fade)
            each = len(weights) // len(blocks)
            product = 0.0
            for i, block in enumerate(blocks):
                probs = jnp.concatenate(weights[i * each : (i + 1) * each], axis=1)
                product = product + jnp.dot(
                    probs.astype(jnp.bfloat16), block, preferred_element_type=jnp.float32
                )
            acc[part] = acc[part] * jnp.tile(fade, (1, channels // lanes)) + product

    steps = own_steps + (far - 1) * chunks + half_chunks
    first = own_steps + primed - lead
    taper = first + 3

    @pl.loop(0, steps - 1)
    def _(s):
        @pl.when(jnp.logical_and(s >= first, s < taper))
        def _():
            relay(s + lead)

        @pl.when(s >= taper + lead)
        def _():
            relay(s)

        arrived(1, s)
        blocks = []
        for way in (0, 1):
            d, zb, k = spot(way, s)
            blocks.append(kv[zb, k].reshape(2 * chunk, channels))
        attend(blocks)

    final = [spot(way, steps - 1) for way in (0, 1)]
    relay(steps - 1)
    attend([jnp.concatenate([kv[zb, k, c] for d, zb, k in final], axis=0)])
    arrived(1, steps - 1)
    attend([jnp.concatenate([kv[zb, k, 1 - c] for d, zb, k in final], axis=0)])

    denominator = jnp.sum(total[...], axis=1, keepdims=True)
    average = (acc[...] * (1.0 / denominator) - centre) * gain + attn_shift
    attended = jnp.dot(
        average.astype(jnp.bfloat16), wvo[...], preferred_element_type=jnp.float32
    )
    field = (own().reshape(rows, channels).astype(jnp.float32) + attended).astype(jnp.bfloat16)
    hidden[...] = field
    share_moments(1, field.astype(jnp.float32))

    up = pltpu.make_async_remote_copy(
        src_ref=hidden.at[pl.ds(0, wide)],
        dst_ref=halo.at[1],
        send_sem=halo_send.at[1],
        recv_sem=halo_recv.at[1],
        device_id=(img, r - 1),
        device_id_type=MESH,
    )
    down = pltpu.make_async_remote_copy(
        src_ref=hidden.at[pl.ds(rows - wide, wide)],
        dst_ref=halo.at[0],
        send_sem=halo_send.at[0],
        recv_sem=halo_recv.at[0],
        device_id=(img, r + 1),
        device_id_type=MESH,
    )

    @pl.when(r > 0)
    def _():
        up.start()

    @pl.when(r < n - 1)
    def _():
        down.start()

    along = kv.at[pl.ds(0, (steps - own_steps) // 2), pl.ds(0, 1)]
    across = kv.at[pl.ds(0, deep // 2)]
    for way, view in enumerate((along, along, across)):
        whole(view, send_sem.at[way], recv_sem.at[0, 0]).wait_send()

    filled(wc, weight_sem.at[2])
    centre, scale = gather_moments(1)
    gain = scale * conv_gain

    def activate(values):
        v = (values.astype(jnp.float32) - centre) * gain + conv_shift
        return (v / (1.0 + jnp.exp(-v))).astype(jnp.bfloat16)

    order = [*range(1, lines - 1), 0, lines - 1]

    def place(line, values):
        for dy in range(3):
            y = line + 1 - dy
            if 0 <= y < lines:
                slot = order.index(y) * wide
                stacked[slot : slot + wide, dy * channels : (dy + 1) * channels] = values

    def convolve(first, last):
        count = (last - first) * wide
        window = stacked[first * wide : last * wide]
        column = lax.broadcasted_iota(jnp.int32, (count, channels), 0) % wide

        def taps(dx):
            return jnp.dot(window, wc[dx], preferred_element_type=jnp.float32)

        convolved = taps(1) + conv_bias
        convolved = convolved + jnp.where(column > 0, pltpu.roll(taps(0), 1, 0), 0.0)
        convolved = convolved + jnp.where(
            column < wide - 1, pltpu.roll(taps(2), count - 1, 0), 0.0
        )
        for i, y in enumerate(order[first:last]):
            line = slice(y * wide, (y + 1) * wide)
            part = convolved[i * wide : (i + 1) * wide]
            out[line] = (hidden[line].astype(jnp.float32) + part).astype(jnp.bfloat16)

    for line in range(lines):
        place(line, activate(hidden[line * wide : (line + 1) * wide]))
    convolve(0, lines - 2)

    @pl.when(r > 0)
    def _():
        up.wait_send()
        down.wait_recv()
        place(-1, activate(halo[0]))

    @pl.when(r == 0)
    def _():
        place(-1, jnp.zeros((wide, channels), jnp.bfloat16))

    @pl.when(r < n - 1)
    def _():
        down.wait_send()
        up.wait_recv()
        place(lines, activate(halo[1]))

    @pl.when(r == n - 1)
    def _():
        place(lines, jnp.zeros((wide, channels), jnp.bfloat16))

    convolve(lines - 2, lines)

    for which in range(2):
        stat_all(which).wait_send()


def local(n, latent, attn_gain, attn_shift, w_query, w_key, w_value, w_out,
          conv_gain, conv_shift, w_conv, conv_bias):
    height, wide, channels = latent.shape
    rows = height * wide
    chunks = rows // CHUNK
    anywhere = pl.BlockSpec(memory_space=pl.ANY)
    bf16, f32 = jnp.bfloat16, jnp.float32
    square = pltpu.VMEM((channels, channels), bf16)
    dma = pltpu.SemaphoreType.DMA
    def kept(value):
        return pltpu.with_memory_space_constraint(value, pltpu.HBM)

    encoded = pl.pallas_call(
        functools.partial(kernel, n, wide),
        out_shape=jax.ShapeDtypeStruct((rows, channels), bf16),
        in_specs=[anywhere] * 11,
        out_specs=pl.BlockSpec(memory_space=pltpu.VMEM),
        scratch_shapes=[
            pltpu.VMEM((n // 2, chunks, 2, CHUNK, channels), bf16),
            pltpu.VMEM((4, channels, channels), bf16),
            square,
            pltpu.VMEM((3, 3 * channels, channels), bf16),
            square,
            pltpu.VMEM((channels, 128), bf16),
            pltpu.VMEM((128, channels), bf16),
            pltpu.VMEM((2, n, 2, 128), f32),
            pltpu.VMEM((rows, channels), bf16),
            pltpu.VMEM((rows, 128), f32),
            pltpu.VMEM((rows, 128), f32),
            pltpu.VMEM((rows, 128), f32),
            pltpu.VMEM((rows, channels), f32),
            pltpu.VMEM((rows, channels), bf16),
            pltpu.VMEM((2, wide, channels), bf16),
            pltpu.VMEM((rows, 3 * channels), bf16),
            dma((chunks,)),
            dma((3,)),
            dma((3,)),
            dma((2, n)),
            dma((2,)),
            dma((2,)),
            dma((2,)),
            dma((2,)),
            pltpu.VMEM((5, 1, channels), f32),
            dma,
            pltpu.SemaphoreType.REGULAR((n // 4,)),
        ],
        compiler_params=pltpu.CompilerParams(
            collective_id=0, has_side_effects=True, vmem_limit_bytes=48 * 1024 * 1024
        ),
    )(
        *map(kept, (latent.reshape(chunks, CHUNK, channels), w_query, w_key, w_value, w_out, w_conv)),
        *(kept(v.reshape(1, channels)) for v in (attn_gain, attn_shift, conv_gain, conv_shift, conv_bias)),
    )
    return encoded.reshape(height, wide, channels)


def solution(mesh):
    in_specs = (P(("img", "row"), None, None), P(), P(), P(), P(), P(), P(), P(), P(), P(), P())
    out_specs = P(("img", "row"), None, None)
    body = functools.partial(local, mesh.shape["row"])
    return jax.shard_map(body, mesh=mesh, in_specs=in_specs, out_specs=out_specs, check_vma=False)
```

```python
import functools
import math

import jax
import jax.numpy as jnp
from jax import lax
from jax.experimental import pallas as pl
from jax.experimental.pallas import tpu as pltpu
from jax.sharding import PartitionSpec as P

GROUPS = 32
EPS = 1e-06
CHUNK = 128
MESH = pl.DeviceIdType.MESH
LOG2E = math.log2(math.e)
NT = (((1,), (1,)), ((), ()))


def exact_dot(vectors, matrix):
    index = lax.broadcasted_iota(jnp.int32, (16, vectors[0].shape[1]), 0)
    parts = jnp.zeros(index.shape, jnp.float32)
    for i, vector in enumerate(vectors):
        high = vector.astype(jnp.bfloat16).astype(jnp.float32)
        rest = vector - high
        mid = rest.astype(jnp.bfloat16).astype(jnp.float32)
        for j, part in enumerate((high, mid, rest - mid)):
            parts = jnp.where(index == 3 * i + j, part, parts)
    sums = jnp.dot(parts.astype(jnp.bfloat16), matrix, preferred_element_type=jnp.float32)
    return [
        sums[3 * i : 3 * i + 1] + sums[3 * i + 1 : 3 * i + 2] + sums[3 * i + 2 : 3 * i + 3]
        for i in range(len(vectors))
    ]


def kernel(
    n, wide,
    latent, w_query, w_key, w_value, w_out, w_conv,
    attn_gain_in, attn_shift_in, conv_gain_in, conv_shift_in, conv_bias_in,
    out,
    kv, mats, wvo, wc, ones, fold, spread, moments, queries, bias, maxima, total, acc, hidden, halo, stacked,
    load_sem, weight_sem, send_sem, recv_sem, stat_send, stat_recv, halo_send, halo_recv,
    vectors, vector_sem, entered, mixed, edge,
):
    deep, chunks, _, chunk, channels = kv.shape
    rows = chunks * chunk
    far = deep // 2
    half_chunks = chunks // 2
    own_steps = half_chunks
    early = 3
    primed = 3
    lead = 3
    lines = rows // wide
    size = channels // GROUPS
    img = lax.axis_index("img")
    r = lax.axis_index("row")
    z = r // 2
    c = r % 2
    partner = r + 1 - 2 * c

    barrier = pltpu.get_barrier_semaphore()

    upward, downward = lax.rem(r + 2, n), lax.rem(r + n - 2, n)
    for target in (upward, downward, partner):
        pl.semaphore_signal(barrier, inc=1, device_id=(img, target), device_id_type=MESH)

    loads = [
        pltpu.make_async_copy(latent.at[k], kv.at[z, k, c], load_sem.at[k]) for k in range(chunks)
    ]
    for load in loads:
        load.start()
    def filled(view, sem):
        pltpu.make_async_copy(view, view, sem).wait()

    for i, source in enumerate((w_query, w_key, w_value, w_out)):
        pltpu.make_async_copy(source, mats.at[i], weight_sem.at[i // 2]).start()
    for dy in range(3):
        for dx in range(3):
            pltpu.make_async_copy(
                w_conv.at[dy, dx], wc.at[dy, pl.ds(dx * channels, channels)], weight_sem.at[2]
            ).start()
    for i, source in enumerate(
        (attn_gain_in, attn_shift_in, conv_gain_in, conv_shift_in, conv_bias_in)
    ):
        pltpu.make_async_copy(source, vectors.at[i], vector_sem).start()

    def piece(way, zb, k, mark):
        return pltpu.make_async_remote_copy(
            src_ref=kv.at[zb, k, c],
            dst_ref=kv.at[zb, k, c],
            send_sem=send_sem.at[way],
            recv_sem=recv_sem.at[way // 2, mark],
            device_id=(img, (upward, downward, partner)[way]),
            device_id_type=MESH,
        )

    def whole(view, send, recv):
        return pltpu.make_async_remote_copy(
            src_ref=view,
            dst_ref=view,
            send_sem=send,
            recv_sem=recv,
            device_id=(img, partner),
            device_id_type=MESH,
        )

    def arrived(relayed, s):
        pair = kv.at[0, 0]
        whole(pair, send_sem.at[0], recv_sem.at[relayed, s]).wait_recv()

    def stat_copy(which, j):
        return pltpu.make_async_remote_copy(
            src_ref=moments.at[which, r],
            dst_ref=moments.at[which, r],
            send_sem=stat_send.at[which],
            recv_sem=stat_recv.at[which],
            device_id=(img, lax.rem(r + j, n)),
            device_id_type=MESH,
        )

    def stat_all(which):
        view = moments.at[which, pl.ds(0, n - 1)]
        return whole(view, stat_send.at[which], stat_recv.at[which])

    def own():
        return kv[z, :, c]

    def send_own(k):
        piece(0, z, k, own_steps + k).start()
        piece(1, z, k, own_steps + k).start()
        piece(2, z, k, k // 2).start()

    def split(way, d, k):
        part = (k < half_chunks) if way == 0 else (k >= half_chunks)
        return jnp.logical_or(d < far, jnp.logical_and(d == far, part))

    def spot(way, s):
        e = s - own_steps
        d = jnp.where(e < 0, 0, e // chunks + 1)
        last = d == far
        step = jnp.where(e < 0, 2 * s + way, lax.rem(e + chunks, chunks) + jnp.where(last, way * half_chunks, 0))
        zb = lax.rem(z + (deep - d if way == 0 else d), deep)
        return d, zb, step

    def relay(s):
        arrived(0, s)
        for way in (0, 1):
            d, zb, k = spot(way, s)
            mark = s + chunks - jnp.where(d + 1 == far, way * half_chunks, 0)

            @pl.when(split(way, d + 1, k))
            def _(way=way, zb=zb, k=k, mark=mark):
                piece(way, zb, k, mark).start()

            piece(2, zb, k, s).start()

    def share_moments(which, field):
        mean = jnp.sum(field, axis=0, keepdims=True) * (1.0 / rows)
        offset = field - mean
        square = jnp.sum(offset * offset, axis=0, keepdims=True)
        (near,) = exact_dot([mean], ones[...])
        away = mean - near * (1.0 / size)
        sums, squares = exact_dot([mean, square + rows * (away * away)], fold[...])
        moments[which, r, 0:1, :] = sums * (1.0 / size)
        moments[which, r, 1:2, :] = squares

        for j in sorted(range(1, n), key=lambda j: abs(j - n // 2)):
            stat_copy(which, j).start()

    def gather_moments(which):
        stat_all(which).wait_recv()
        every = moments[which]
        means = every[:, 0, :]
        squares = every[:, 1, :]
        centre = jnp.sum(means, axis=0, keepdims=True) * (1.0 / n)
        away = means - centre
        whole = jnp.sum(squares + (rows * size) * (away * away), axis=0, keepdims=True)
        scale = lax.rsqrt(whole * (1.0 / (n * size * rows)) + EPS)
        return exact_dot([centre, scale], spread[...])

    pl.semaphore_wait(barrier, 3)
    for k in range(chunks):
        loads[k].wait()
        if k < early:
            send_own(k)
    def groups(shape, left, right):
        rows_of, columns_of = (lax.broadcasted_iota(jnp.int32, shape, i) for i in (0, 1))
        return jnp.where(rows_of // left == columns_of // right, 1.0, 0.0).astype(jnp.bfloat16)

    def prepare(j):
        if j == 0:
            ones[...] = groups(ones.shape, size, size)
        if j == 1:
            fold[...] = groups(fold.shape, size, 1)
            spread[...] = groups(spread.shape, 1, size)
            maxima[...] = jnp.full_like(maxima, -1e30)
            total[...] = jnp.zeros_like(total)
        if j == 2:
            acc[...] = jnp.zeros_like(acc)

    for j in range(far - 1):
        for target in (upward, downward):
            pl.semaphore_signal(
                entered.at[j], inc=1, device_id=(img, target), device_id_type=MESH
            )
        prepare(j)
        pl.semaphore_wait(entered.at[j], 2)
    pl.semaphore_signal(entered.at[far - 1], inc=1, device_id=(img, partner), device_id_type=MESH)
    pl.semaphore_wait(entered.at[far - 1], 1)
    share_moments(0, own().reshape(rows, channels).astype(jnp.float32))
    for k in range(early, chunks):
        send_own(k)

    for s in range(own_steps, own_steps + primed):
        relay(s)

    filled(mats.at[pl.ds(0, 2)], weight_sem.at[0])
    filled(vectors, vector_sem)
    attn_gain, attn_shift, conv_gain, conv_shift = (vectors[i] for i in range(4))
    conv_bias = vectors[4]
    centre, scale = gather_moments(0)
    gain = scale * attn_gain
    positions = own().reshape(rows, channels).astype(jnp.float32)
    normed = ((positions - centre) * gain + attn_shift).astype(jnp.bfloat16)
    query = jnp.dot(normed, mats[0], preferred_element_type=jnp.float32).astype(jnp.bfloat16)
    folded = lax.dot_general(query, mats[1], NT, preferred_element_type=jnp.float32) * (
        LOG2E / math.sqrt(channels)
    )
    queries[...] = (folded * gain).astype(jnp.bfloat16)
    constant = jnp.sum(folded * (attn_shift - centre * gain), axis=1, keepdims=True)
    bias[...] = jnp.broadcast_to(constant, bias.shape)

    filled(mats.at[pl.ds(2, 2)], weight_sem.at[1])
    wvo[...] = jnp.dot(mats[2], mats[3], preferred_element_type=jnp.float32).astype(jnp.bfloat16)

    filled(wc, weight_sem.at[2])

    @pl.loop(0, 3)
    def _(dx):
        part = pl.ds(pl.multiple_of(dx * channels, channels), channels)
        outer = wc[0, part].astype(jnp.float32) + wc[2, part].astype(jnp.float32)
        inner = wc[1, part].astype(jnp.float32)
        mixed[0, part] = (0.5 * (outer + inner)).astype(jnp.bfloat16)
        mixed[1, part] = (0.5 * (outer - inner)).astype(jnp.bfloat16)

    lanes = 128
    halves = [slice(i, i + rows // 2) for i in range(0, rows, rows // 2)]

    def attend(blocks):
        scores = [
            [
                lax.dot_general(queries[part], block, NT, preferred_element_type=jnp.float32)
                for block in blocks
            ]
            for part in halves
        ]
        for part, pair in zip(halves, scores):
            columns = [
                score[:, j : j + lanes] for score in pair for j in range(0, 2 * chunk, lanes)
            ]
            peak = functools.reduce(jnp.maximum, columns)
            offset = bias[part]
            newest = jnp.maximum(maxima[part], jnp.max(peak, axis=1, keepdims=True) + offset)
            fade = jnp.exp2(maxima[part] - newest)
            maxima[part] = newest
            level = newest - offset
            weights = [jnp.exp2(column - level) for column in columns]
            total[part] = functools.reduce(jnp.add, weights, total[part] * fade)
            each = len(weights) // len(blocks)
            product = 0.0
            for i, block in enumerate(blocks):
                probs = jnp.concatenate(weights[i * each : (i + 1) * each], axis=1)
                product = product + jnp.dot(
                    probs.astype(jnp.bfloat16), block, preferred_element_type=jnp.float32
                )
            acc[part] = acc[part] * jnp.tile(fade, (1, channels // lanes)) + product

    steps = own_steps + (far - 1) * chunks + half_chunks
    first = own_steps + primed - lead
    taper = first + 3

    @pl.loop(0, steps - 1)
    def _(s):
        @pl.when(jnp.logical_and(s >= first, s < taper))
        def _():
            relay(s + lead)

        @pl.when(s >= taper + lead)
        def _():
            relay(s)

        arrived(1, s)
        blocks = []
        for way in (0, 1):
            d, zb, k = spot(way, s)
            blocks.append(kv[zb, k].reshape(2 * chunk, channels))
        attend(blocks)

    final = [spot(way, steps - 1) for way in (0, 1)]
    relay(steps - 1)
    attend([jnp.concatenate([kv[zb, k, c] for d, zb, k in final], axis=0)])
    arrived(1, steps - 1)
    attend([jnp.concatenate([kv[zb, k, 1 - c] for d, zb, k in final], axis=0)])

    denominator = jnp.sum(total[...], axis=1, keepdims=True)
    average = (acc[...] * (1.0 / denominator) - centre) * gain + attn_shift
    attended = jnp.dot(
        average.astype(jnp.bfloat16), wvo[...], preferred_element_type=jnp.float32
    )
    field = (own().reshape(rows, channels).astype(jnp.float32) + attended).astype(jnp.bfloat16)
    hidden[...] = field
    share_moments(1, field.astype(jnp.float32))

    up = pltpu.make_async_remote_copy(
        src_ref=hidden.at[pl.ds(0, wide)],
        dst_ref=halo.at[1],
        send_sem=halo_send.at[1],
        recv_sem=halo_recv.at[1],
        device_id=(img, r - 1),
        device_id_type=MESH,
    )
    down = pltpu.make_async_remote_copy(
        src_ref=hidden.at[pl.ds(rows - wide, wide)],
        dst_ref=halo.at[0],
        send_sem=halo_send.at[0],
        recv_sem=halo_recv.at[0],
        device_id=(img, r + 1),
        device_id_type=MESH,
    )

    @pl.when(r > 0)
    def _():
        up.start()

    @pl.when(r < n - 1)
    def _():
        down.start()

    along = kv.at[pl.ds(0, (steps - own_steps) // 2), pl.ds(0, 1)]
    across = kv.at[pl.ds(0, deep // 2)]
    for way, view in enumerate((along, along, across)):
        whole(view, send_sem.at[way], recv_sem.at[0, 0]).wait_send()

    centre, scale = gather_moments(1)
    gain = scale * conv_gain

    def activate(values):
        v = (values.astype(jnp.float32) - centre) * gain + conv_shift
        return (v / (1.0 + jnp.exp(-v))).astype(jnp.bfloat16).astype(jnp.float32)

    column = lax.broadcasted_iota(jnp.int32, (wide, channels), 0)

    def place(term, pair, values):
        at = slice(pair * wide, (pair + 1) * wide)
        before = jnp.where(column > 0, pltpu.roll(values, 1, 0), 0.0)
        after = jnp.where(column < wide - 1, pltpu.roll(values, wide - 1, 0), 0.0)
        for dx, part in enumerate((before, values, after)):
            stacked[term, at, dx * channels : (dx + 1) * channels] = part.astype(jnp.bfloat16)

    def product(term, matrix):
        return jnp.dot(stacked[term], matrix, preferred_element_type=jnp.float32)

    first, second, third, fourth = (
        activate(hidden[y * wide : (y + 1) * wide]) for y in range(lines)
    )
    edge[0] = second
    edge[1] = third
    for pair, (upper, lower) in enumerate(((first, second), (third, fourth))):
        place(1, pair, upper + lower)
        place(2, pair, lower - upper)
    place(0, 1, second - fourth)
    place(3, 0, first - third)
    sums, gaps = product(1, mixed[0]), product(2, mixed[1])
    acc[: rows // 2] = sums + gaps
    acc[rows // 2 :] = sums - gaps

    @pl.when(r > 0)
    def _():
        up.wait_send()
        down.wait_recv()
        edge[2] = activate(halo[0])

    @pl.when(r == 0)
    def _():
        edge[2] = jnp.zeros((wide, channels), jnp.float32)

    @pl.when(r < n - 1)
    def _():
        down.wait_send()
        up.wait_recv()
        edge[3] = activate(halo[1])

    @pl.when(r == n - 1)
    def _():
        edge[3] = jnp.zeros((wide, channels), jnp.float32)

    place(0, 0, edge[2] - edge[0])
    place(3, 1, edge[1] - edge[3])
    evens = acc[: rows // 2] + product(0, wc[0])
    odds = acc[rows // 2 :] - product(3, wc[2])
    for parity, values in enumerate((evens, odds)):
        for pair in range(2):
            y = 2 * pair + parity
            line = slice(y * wide, (y + 1) * wide)
            part = values[pair * wide : (pair + 1) * wide] + conv_bias
            out[line] = (hidden[line].astype(jnp.float32) + part).astype(jnp.bfloat16)

    for which in range(2):
        stat_all(which).wait_send()


def local(n, latent, attn_gain, attn_shift, w_query, w_key, w_value, w_out,
          conv_gain, conv_shift, w_conv, conv_bias):
    height, wide, channels = latent.shape
    rows = height * wide
    chunks = rows // CHUNK
    anywhere = pl.BlockSpec(memory_space=pl.ANY)
    bf16, f32 = jnp.bfloat16, jnp.float32
    square = pltpu.VMEM((channels, channels), bf16)
    dma = pltpu.SemaphoreType.DMA
    def kept(value):
        return pltpu.with_memory_space_constraint(value, pltpu.HBM)

    encoded = pl.pallas_call(
        functools.partial(kernel, n, wide),
        out_shape=jax.ShapeDtypeStruct((rows, channels), bf16),
        in_specs=[anywhere] * 11,
        out_specs=pl.BlockSpec(memory_space=pltpu.VMEM),
        scratch_shapes=[
            pltpu.VMEM((n // 2, chunks, 2, CHUNK, channels), bf16),
            pltpu.VMEM((4, channels, channels), bf16),
            square,
            pltpu.VMEM((3, 3 * channels, channels), bf16),
            square,
            pltpu.VMEM((channels, 128), bf16),
            pltpu.VMEM((128, channels), bf16),
            pltpu.VMEM((2, n, 2, 128), f32),
            pltpu.VMEM((rows, channels), bf16),
            pltpu.VMEM((rows, 128), f32),
            pltpu.VMEM((rows, 128), f32),
            pltpu.VMEM((rows, 128), f32),
            pltpu.VMEM((rows, channels), f32),
            pltpu.VMEM((rows, channels), bf16),
            pltpu.VMEM((2, wide, channels), bf16),
            pltpu.VMEM((4, rows // 2, 3 * channels), bf16),
            dma((chunks,)),
            dma((3,)),
            dma((3,)),
            dma((2, n)),
            dma((2,)),
            dma((2,)),
            dma((2,)),
            dma((2,)),
            pltpu.VMEM((5, 1, channels), f32),
            dma,
            pltpu.SemaphoreType.REGULAR((n // 4,)),
            pltpu.VMEM((2, 3 * channels, channels), bf16),
            pltpu.VMEM((4, wide, channels), f32),
        ],
        compiler_params=pltpu.CompilerParams(
            collective_id=0, has_side_effects=True, vmem_limit_bytes=48 * 1024 * 1024
        ),
    )(
        *map(kept, (latent.reshape(chunks, CHUNK, channels), w_query, w_key, w_value, w_out, w_conv)),
        *(kept(v.reshape(1, channels)) for v in (attn_gain, attn_shift, conv_gain, conv_shift, conv_bias)),
    )
    return encoded.reshape(height, wide, channels)


def solution(mesh):
    in_specs = (P(("img", "row"), None, None), P(), P(), P(), P(), P(), P(), P(), P(), P(), P())
    out_specs = P(("img", "row"), None, None)
    body = functools.partial(local, mesh.shape["row"])
    return jax.shard_map(body, mesh=mesh, in_specs=in_specs, out_specs=out_specs, check_vma=False)
```

```python
import functools
import math

import jax
import jax.numpy as jnp
from jax import lax
from jax.experimental import pallas as pl
from jax.experimental.pallas import tpu as pltpu
from jax.sharding import PartitionSpec as P

GROUPS = 32
EPS = 1e-06
CHUNK = 128
MESH = pl.DeviceIdType.MESH
LOG2E = math.log2(math.e)
NT = (((1,), (1,)), ((), ()))


def exact_dot(vectors, matrix):
    index = lax.broadcasted_iota(jnp.int32, (16, vectors[0].shape[1]), 0)
    parts = jnp.zeros(index.shape, jnp.float32)
    for i, vector in enumerate(vectors):
        high = vector.astype(jnp.bfloat16).astype(jnp.float32)
        rest = vector - high
        mid = rest.astype(jnp.bfloat16).astype(jnp.float32)
        for j, part in enumerate((high, mid, rest - mid)):
            parts = jnp.where(index == 3 * i + j, part, parts)
    sums = jnp.dot(parts.astype(jnp.bfloat16), matrix, preferred_element_type=jnp.float32)
    return [
        sums[3 * i : 3 * i + 1] + sums[3 * i + 1 : 3 * i + 2] + sums[3 * i + 2 : 3 * i + 3]
        for i in range(len(vectors))
    ]


def kernel(
    n, wide,
    latent, w_query, w_key, w_value, w_out, w_conv,
    attn_gain_in, attn_shift_in, conv_gain_in, conv_shift_in, conv_bias_in,
    out,
    kv, mats, wvo, wc, ones, fold, spread, moments, queries, bias, maxima, total, acc, hidden, halo, stacked,
    load_sem, weight_sem, send_sem, recv_sem, stat_send, stat_recv, halo_send, halo_recv,
    vectors, vector_sem, entered, mixed, edge,
):
    deep, chunks, _, chunk, channels = kv.shape
    rows = chunks * chunk
    far = deep // 2
    half_chunks = chunks // 2
    own_steps = half_chunks
    early = 3
    primed = 3
    lead = 3
    lines = rows // wide
    size = channels // GROUPS
    img = lax.axis_index("img")
    r = lax.axis_index("row")
    z = r // 2
    c = r % 2
    partner = r + 1 - 2 * c

    barrier = pltpu.get_barrier_semaphore()

    upward, downward = lax.rem(r + 2, n), lax.rem(r + n - 2, n)
    for target in (upward, downward, partner):
        pl.semaphore_signal(barrier, inc=1, device_id=(img, target), device_id_type=MESH)

    loads = [
        pltpu.make_async_copy(latent.at[k], kv.at[z, k, c], load_sem.at[k]) for k in range(chunks)
    ]
    for load in loads:
        load.start()
    def filled(view, sem):
        pltpu.make_async_copy(view, view, sem).wait()

    for i, source in enumerate((w_query, w_key, w_value, w_out)):
        pltpu.make_async_copy(source, mats.at[i], weight_sem.at[i // 2]).start()
    for dy in range(3):
        for dx in range(3):
            pltpu.make_async_copy(
                w_conv.at[dy, dx], wc.at[dy, pl.ds(dx * channels, channels)], weight_sem.at[2]
            ).start()
    for i, source in enumerate(
        (attn_gain_in, attn_shift_in, conv_gain_in, conv_shift_in, conv_bias_in)
    ):
        pltpu.make_async_copy(source, vectors.at[i], vector_sem).start()

    def piece(way, zb, k, mark):
        return pltpu.make_async_remote_copy(
            src_ref=kv.at[zb, k, c],
            dst_ref=kv.at[zb, k, c],
            send_sem=send_sem.at[way],
            recv_sem=recv_sem.at[way // 2, mark],
            device_id=(img, (upward, downward, partner)[way]),
            device_id_type=MESH,
        )

    def whole(view, send, recv):
        return pltpu.make_async_remote_copy(
            src_ref=view,
            dst_ref=view,
            send_sem=send,
            recv_sem=recv,
            device_id=(img, partner),
            device_id_type=MESH,
        )

    def arrived(relayed, s):
        pair = kv.at[0, 0]
        whole(pair, send_sem.at[0], recv_sem.at[relayed, s]).wait_recv()

    def stat_copy(which, j):
        return pltpu.make_async_remote_copy(
            src_ref=moments.at[which, r],
            dst_ref=moments.at[which, r],
            send_sem=stat_send.at[which],
            recv_sem=stat_recv.at[which],
            device_id=(img, lax.rem(r + j, n)),
            device_id_type=MESH,
        )

    def stat_all(which):
        view = moments.at[which, pl.ds(0, n - 1)]
        return whole(view, stat_send.at[which], stat_recv.at[which])

    def own():
        return kv[z, :, c]

    def send_own(k):
        piece(0, z, k, own_steps + k).start()
        piece(1, z, k, own_steps + k).start()
        piece(2, z, k, k // 2).start()

    def split(way, d, k):
        part = (k < half_chunks) if way == 0 else (k >= half_chunks)
        return jnp.logical_or(d < far, jnp.logical_and(d == far, part))

    def spot(way, s):
        e = s - own_steps
        d = jnp.where(e < 0, 0, e // chunks + 1)
        last = d == far
        step = jnp.where(e < 0, 2 * s + way, lax.rem(e + chunks, chunks) + jnp.where(last, way * half_chunks, 0))
        zb = lax.rem(z + (deep - d if way == 0 else d), deep)
        return d, zb, step

    def relay(s):
        arrived(0, s)
        for way in (0, 1):
            d, zb, k = spot(way, s)
            mark = s + chunks - jnp.where(d + 1 == far, way * half_chunks, 0)

            @pl.when(split(way, d + 1, k))
            def _(way=way, zb=zb, k=k, mark=mark):
                piece(way, zb, k, mark).start()

            piece(2, zb, k, s).start()

    def share_moments(which, field):
        mean = jnp.sum(field, axis=0, keepdims=True) * (1.0 / rows)
        offset = field - mean
        square = jnp.sum(offset * offset, axis=0, keepdims=True)
        (near,) = exact_dot([mean], ones[...])
        away = mean - near * (1.0 / size)
        sums, squares = exact_dot([mean, square + rows * (away * away)], fold[...])
        moments[which, r, 0:1, :] = sums * (1.0 / size)
        moments[which, r, 1:2, :] = squares

        for j in sorted(range(1, n), key=lambda j: abs(j - n // 2)):
            stat_copy(which, j).start()

    def gather_moments(which):
        stat_all(which).wait_recv()
        every = moments[which]
        means = every[:, 0, :]
        squares = every[:, 1, :]
        centre = jnp.sum(means, axis=0, keepdims=True) * (1.0 / n)
        away = means - centre
        whole = jnp.sum(squares + (rows * size) * (away * away), axis=0, keepdims=True)
        scale = lax.rsqrt(whole * (1.0 / (n * size * rows)) + EPS)
        return exact_dot([centre, scale], spread[...])

    pl.semaphore_wait(barrier, 3)
    for k in range(chunks):
        loads[k].wait()
        if k < early:
            send_own(k)
    def groups(shape, left, right):
        rows_of, columns_of = (lax.broadcasted_iota(jnp.int32, shape, i) for i in (0, 1))
        return jnp.where(rows_of // left == columns_of // right, 1.0, 0.0).astype(jnp.bfloat16)

    def prepare(j):
        if j == 0:
            ones[...] = groups(ones.shape, size, size)
        if j == 1:
            fold[...] = groups(fold.shape, size, 1)
            spread[...] = groups(spread.shape, 1, size)
            maxima[...] = jnp.full_like(maxima, -1e30)
            total[...] = jnp.zeros_like(total)
        if j == 2:
            acc[...] = jnp.zeros_like(acc)

    for j in range(far - 1):
        for target in (upward, downward):
            pl.semaphore_signal(
                entered.at[j], inc=1, device_id=(img, target), device_id_type=MESH
            )
        prepare(j)
        pl.semaphore_wait(entered.at[j], 2)
    pl.semaphore_signal(entered.at[far - 1], inc=1, device_id=(img, partner), device_id_type=MESH)
    pl.semaphore_wait(entered.at[far - 1], 1)
    share_moments(0, own().reshape(rows, channels).astype(jnp.float32))
    for k in range(early, chunks):
        send_own(k)

    for s in range(own_steps, own_steps + primed):
        relay(s)

    filled(mats.at[pl.ds(0, 2)], weight_sem.at[0])
    filled(vectors, vector_sem)
    attn_gain, attn_shift, conv_gain, conv_shift = (vectors[i] for i in range(4))
    conv_bias = vectors[4]
    centre, scale = gather_moments(0)
    gain = scale * attn_gain
    positions = own().reshape(rows, channels).astype(jnp.float32)
    normed = ((positions - centre) * gain + attn_shift).astype(jnp.bfloat16)
    query = jnp.dot(normed, mats[0], preferred_element_type=jnp.float32).astype(jnp.bfloat16)
    folded = lax.dot_general(query, mats[1], NT, preferred_element_type=jnp.float32) * (
        LOG2E / math.sqrt(channels)
    )
    queries[...] = (folded * gain).astype(jnp.bfloat16)
    constant = jnp.sum(folded * (attn_shift - centre * gain), axis=1, keepdims=True)
    bias[...] = jnp.broadcast_to(constant, bias.shape)

    filled(mats.at[pl.ds(2, 2)], weight_sem.at[1])
    wvo[...] = jnp.dot(mats[2], mats[3], preferred_element_type=jnp.float32).astype(jnp.bfloat16)

    filled(wc, weight_sem.at[2])

    @pl.loop(0, 3)
    def _(dx):
        part = pl.ds(pl.multiple_of(dx * channels, channels), channels)
        outer = wc[0, part].astype(jnp.float32) + wc[2, part].astype(jnp.float32)
        inner = wc[1, part].astype(jnp.float32)
        mixed[0, part] = (0.5 * (outer + inner)).astype(jnp.bfloat16)
        mixed[1, part] = (0.5 * (outer - inner)).astype(jnp.bfloat16)

    lanes = 128
    halves = [slice(i, i + rows // 2) for i in range(0, rows, rows // 2)]

    def attend(blocks):
        scores = [
            [
                lax.dot_general(queries[part], block, NT, preferred_element_type=jnp.float32)
                for block in blocks
            ]
            for part in halves
        ]
        for part, pair in zip(halves, scores):
            columns = [
                score[:, j : j + lanes] for score in pair for j in range(0, 2 * chunk, lanes)
            ]
            peak = functools.reduce(jnp.maximum, columns)
            offset = bias[part]
            newest = jnp.maximum(maxima[part], jnp.max(peak, axis=1, keepdims=True) + offset)
            fade = jnp.exp2(maxima[part] - newest)
            maxima[part] = newest
            level = newest - offset
            weights = [jnp.exp2(column - level) for column in columns]
            total[part] = functools.reduce(jnp.add, weights, total[part] * fade)
            each = len(weights) // len(blocks)
            product = 0.0
            for i, block in enumerate(blocks):
                probs = jnp.concatenate(weights[i * each : (i + 1) * each], axis=1)
                product = product + jnp.dot(
                    probs.astype(jnp.bfloat16), block, preferred_element_type=jnp.float32
                )
            acc[part] = acc[part] * jnp.tile(fade, (1, channels // lanes)) + product

    steps = own_steps + (far - 1) * chunks + half_chunks
    first = own_steps + primed - lead
    taper = first + 3

    @pl.loop(0, steps - 1)
    def _(s):
        @pl.when(jnp.logical_and(s >= first, s < taper))
        def _():
            relay(s + lead)

        @pl.when(s >= taper + lead)
        def _():
            relay(s)

        arrived(1, s)
        blocks = []
        for way in (0, 1):
            d, zb, k = spot(way, s)
            blocks.append(kv[zb, k].reshape(2 * chunk, channels))
        attend(blocks)

    final = [spot(way, steps - 1) for way in (0, 1)]
    relay(steps - 1)
    attend([jnp.concatenate([kv[zb, k, c] for d, zb, k in final], axis=0)])
    arrived(1, steps - 1)
    attend([jnp.concatenate([kv[zb, k, 1 - c] for d, zb, k in final], axis=0)])

    denominator = jnp.sum(total[...], axis=1, keepdims=True)
    average = (acc[...] * (1.0 / denominator) - centre) * gain + attn_shift
    attended = jnp.dot(
        average.astype(jnp.bfloat16), wvo[...], preferred_element_type=jnp.float32
    )
    field = (own().reshape(rows, channels).astype(jnp.float32) + attended).astype(jnp.bfloat16)
    hidden[...] = field
    share_moments(1, field.astype(jnp.float32))

    up = pltpu.make_async_remote_copy(
        src_ref=hidden.at[pl.ds(0, wide)],
        dst_ref=halo.at[1],
        send_sem=halo_send.at[1],
        recv_sem=halo_recv.at[1],
        device_id=(img, lax.rem(r + n - 1, n)),
        device_id_type=MESH,
    )
    down = pltpu.make_async_remote_copy(
        src_ref=hidden.at[pl.ds(rows - wide, wide)],
        dst_ref=halo.at[0],
        send_sem=halo_send.at[0],
        recv_sem=halo_recv.at[0],
        device_id=(img, lax.rem(r + 1, n)),
        device_id_type=MESH,
    )

    @pl.when(r > 0)
    def _():
        up.start()

    @pl.when(r < n - 1)
    def _():
        down.start()

    along = kv.at[pl.ds(0, (steps - own_steps) // 2), pl.ds(0, 1)]
    across = kv.at[pl.ds(0, deep // 2)]
    for way, view in enumerate((along, along, across)):
        whole(view, send_sem.at[way], recv_sem.at[0, 0]).wait_send()

    centre, scale = gather_moments(1)
    gain = scale * conv_gain

    def activate(values):
        v = (values.astype(jnp.float32) - centre) * gain + conv_shift
        return (v / (1.0 + jnp.exp(-v))).astype(jnp.bfloat16).astype(jnp.float32)

    column = lax.broadcasted_iota(jnp.int32, (wide, channels), 0)

    def place(term, pair, values):
        at = slice(pair * wide, (pair + 1) * wide)
        before = jnp.where(column > 0, pltpu.roll(values, 1, 0), 0.0)
        after = jnp.where(column < wide - 1, pltpu.roll(values, wide - 1, 0), 0.0)
        for dx, part in enumerate((before, values, after)):
            stacked[term, at, dx * channels : (dx + 1) * channels] = part.astype(jnp.bfloat16)

    def product(term, matrix):
        return jnp.dot(stacked[term], matrix, preferred_element_type=jnp.float32)

    first, second, third, fourth = (
        activate(hidden[y * wide : (y + 1) * wide]) for y in range(lines)
    )
    edge[0] = second
    edge[1] = third
    for pair, (upper, lower) in enumerate(((first, second), (third, fourth))):
        place(1, pair, upper + lower)
        place(2, pair, lower - upper)
    place(0, 1, second - fourth)
    place(3, 0, first - third)
    sums, gaps = product(1, mixed[0]), product(2, mixed[1])
    acc[: rows // 2] = sums + gaps
    acc[rows // 2 :] = sums - gaps

    @pl.when(r > 0)
    def _():
        up.wait_send()
        down.wait_recv()
        edge[2] = activate(halo[0])

    @pl.when(r == 0)
    def _():
        edge[2] = jnp.zeros((wide, channels), jnp.float32)

    @pl.when(r < n - 1)
    def _():
        down.wait_send()
        up.wait_recv()
        edge[3] = activate(halo[1])

    @pl.when(r == n - 1)
    def _():
        edge[3] = jnp.zeros((wide, channels), jnp.float32)

    place(0, 0, edge[2] - edge[0])
    place(3, 1, edge[1] - edge[3])
    evens = acc[: rows // 2] + product(0, wc[0])
    odds = acc[rows // 2 :] - product(3, wc[2])
    for parity, values in enumerate((evens, odds)):
        for pair in range(2):
            y = 2 * pair + parity
            line = slice(y * wide, (y + 1) * wide)
            part = values[pair * wide : (pair + 1) * wide] + conv_bias
            out[line] = (hidden[line].astype(jnp.float32) + part).astype(jnp.bfloat16)

    for which in range(2):
        stat_all(which).wait_send()


def local(n, latent, attn_gain, attn_shift, w_query, w_key, w_value, w_out,
          conv_gain, conv_shift, w_conv, conv_bias):
    height, wide, channels = latent.shape
    rows = height * wide
    chunks = rows // CHUNK
    anywhere = pl.BlockSpec(memory_space=pl.ANY)
    bf16, f32 = jnp.bfloat16, jnp.float32
    square = pltpu.VMEM((channels, channels), bf16)
    dma = pltpu.SemaphoreType.DMA
    def kept(value):
        return pltpu.with_memory_space_constraint(value, pltpu.HBM)

    encoded = pl.pallas_call(
        functools.partial(kernel, n, wide),
        out_shape=jax.ShapeDtypeStruct((rows, channels), bf16),
        in_specs=[anywhere] * 11,
        out_specs=pl.BlockSpec(memory_space=pltpu.VMEM),
        scratch_shapes=[
            pltpu.VMEM((n // 2, chunks, 2, CHUNK, channels), bf16),
            pltpu.VMEM((4, channels, channels), bf16),
            square,
            pltpu.VMEM((3, 3 * channels, channels), bf16),
            square,
            pltpu.VMEM((channels, 128), bf16),
            pltpu.VMEM((128, channels), bf16),
            pltpu.VMEM((2, n, 2, 128), f32),
            pltpu.VMEM((rows, channels), bf16),
            pltpu.VMEM((rows, 128), f32),
            pltpu.VMEM((rows, 128), f32),
            pltpu.VMEM((rows, 128), f32),
            pltpu.VMEM((rows, channels), f32),
            pltpu.VMEM((rows, channels), bf16),
            pltpu.VMEM((2, wide, channels), bf16),
            pltpu.VMEM((4, rows // 2, 3 * channels), bf16),
            dma((chunks,)),
            dma((3,)),
            dma((3,)),
            dma((2, n)),
            dma((2,)),
            dma((2,)),
            dma((2,)),
            dma((2,)),
            pltpu.VMEM((5, 1, channels), f32),
            dma,
            pltpu.SemaphoreType.REGULAR((n // 4,)),
            pltpu.VMEM((2, 3 * channels, channels), bf16),
            pltpu.VMEM((4, wide, channels), f32),
        ],
        compiler_params=pltpu.CompilerParams(
            collective_id=0, has_side_effects=True, vmem_limit_bytes=48 * 1024 * 1024
        ),
    )(
        *map(kept, (latent.reshape(chunks, CHUNK, channels), w_query, w_key, w_value, w_out, w_conv)),
        *(kept(v.reshape(1, channels)) for v in (attn_gain, attn_shift, conv_gain, conv_shift, conv_bias)),
    )
    return encoded.reshape(height, wide, channels)


def solution(mesh):
    in_specs = (P(("img", "row"), None, None), P(), P(), P(), P(), P(), P(), P(), P(), P(), P())
    out_specs = P(("img", "row"), None, None)
    body = functools.partial(local, mesh.shape["row"])
    return jax.shard_map(body, mesh=mesh, in_specs=in_specs, out_specs=out_specs, check_vma=False)
```

```python
import functools
import math

import jax
import jax.numpy as jnp
from jax import lax
from jax.experimental import pallas as pl
from jax.experimental.pallas import tpu as pltpu
from jax.sharding import PartitionSpec as P

GROUPS = 32
EPS = 1e-06
CHUNK = 128
MESH = pl.DeviceIdType.MESH
LOG2E = math.log2(math.e)
NT = (((1,), (1,)), ((), ()))


def exact_dot(vectors, matrix):
    index = lax.broadcasted_iota(jnp.int32, (16, vectors[0].shape[1]), 0)
    parts = jnp.zeros(index.shape, jnp.float32)
    for i, vector in enumerate(vectors):
        high = vector.astype(jnp.bfloat16).astype(jnp.float32)
        rest = vector - high
        mid = rest.astype(jnp.bfloat16).astype(jnp.float32)
        for j, part in enumerate((high, mid, rest - mid)):
            parts = jnp.where(index == 3 * i + j, part, parts)
    sums = jnp.dot(parts.astype(jnp.bfloat16), matrix, preferred_element_type=jnp.float32)
    return [
        sums[3 * i : 3 * i + 1] + sums[3 * i + 1 : 3 * i + 2] + sums[3 * i + 2 : 3 * i + 3]
        for i in range(len(vectors))
    ]


def kernel(
    n, wide,
    latent, w_query, w_key, w_value, w_out, w_conv,
    attn_gain_in, attn_shift_in, conv_gain_in, conv_shift_in, conv_bias_in,
    out,
    kv, mats, wvo, wc, ones, fold, spread, moments, queries, bias, maxima, total, acc, hidden, halo, stacked,
    load_sem, weight_sem, send_sem, recv_sem, stat_send, stat_recv, halo_send, halo_recv,
    vectors, vector_sem, entered, mixed, edge,
):
    deep, chunks, _, chunk, channels = kv.shape
    rows = chunks * chunk
    far = deep // 2
    half_chunks = chunks // 2
    own_steps = half_chunks
    early = 3
    primed = 3
    lead = 3
    lines = rows // wide
    size = channels // GROUPS
    img = lax.axis_index("img")
    r = lax.axis_index("row")
    z = r // 2
    c = r % 2
    partner = r + 1 - 2 * c

    barrier = pltpu.get_barrier_semaphore()

    upward, downward = lax.rem(r + 2, n), lax.rem(r + n - 2, n)
    for target in (upward, downward, partner):
        pl.semaphore_signal(barrier, inc=1, device_id=(img, target), device_id_type=MESH)

    loads = [
        pltpu.make_async_copy(latent.at[k], kv.at[z, k, c], load_sem) for k in range(chunks)
    ]
    for load in loads:
        load.start()
    def filled(view, sem):
        pltpu.make_async_copy(view, view, sem).wait()

    for i, source in enumerate((w_query, w_key, w_value, w_out)):
        pltpu.make_async_copy(source, mats.at[i], weight_sem.at[i // 2]).start()
    for dy in range(3):
        for dx in range(3):
            pltpu.make_async_copy(
                w_conv.at[dy, dx], wc.at[dy, pl.ds(dx * channels, channels)], weight_sem.at[2]
            ).start()
    for i, source in enumerate(
        (attn_gain_in, attn_shift_in, conv_gain_in, conv_shift_in, conv_bias_in)
    ):
        pltpu.make_async_copy(source, vectors.at[i], vector_sem).start()

    def piece(way, zb, k, mark):
        return pltpu.make_async_remote_copy(
            src_ref=kv.at[zb, k, c],
            dst_ref=kv.at[zb, k, c],
            send_sem=send_sem.at[way],
            recv_sem=recv_sem.at[way // 2, mark],
            device_id=(img, (upward, downward, partner)[way]),
            device_id_type=MESH,
        )

    def whole(view, send, recv):
        return pltpu.make_async_remote_copy(
            src_ref=view,
            dst_ref=view,
            send_sem=send,
            recv_sem=recv,
            device_id=(img, partner),
            device_id_type=MESH,
        )

    def arrived(relayed, s):
        pair = kv.at[0, 0]
        whole(pair, send_sem.at[0], recv_sem.at[relayed, s]).wait_recv()

    def stat_copy(which, j):
        return pltpu.make_async_remote_copy(
            src_ref=moments.at[which, r],
            dst_ref=moments.at[which, r],
            send_sem=stat_send.at[which],
            recv_sem=stat_recv.at[which],
            device_id=(img, lax.rem(r + j, n)),
            device_id_type=MESH,
        )

    def stat_all(which):
        view = moments.at[which, pl.ds(0, n - 1)]
        return whole(view, stat_send.at[which], stat_recv.at[which])

    def own():
        return kv[z, :, c]

    def send_own(k):
        piece(0, z, k, own_steps + k).start()
        piece(1, z, k, own_steps + k).start()
        piece(2, z, k, k // 2).start()

    def split(way, d, k):
        part = (k < half_chunks) if way == 0 else (k >= half_chunks)
        return jnp.logical_or(d < far, jnp.logical_and(d == far, part))

    def spot(way, s):
        e = s - own_steps
        d = jnp.where(e < 0, 0, e // chunks + 1)
        last = d == far
        step = jnp.where(e < 0, 2 * s + way, lax.rem(e + chunks, chunks) + jnp.where(last, way * half_chunks, 0))
        zb = lax.rem(z + (deep - d if way == 0 else d), deep)
        return d, zb, step

    def relay(s):
        arrived(0, s)
        for way in (0, 1):
            d, zb, k = spot(way, s)
            mark = s + chunks - jnp.where(d + 1 == far, way * half_chunks, 0)

            @pl.when(split(way, d + 1, k))
            def _(way=way, zb=zb, k=k, mark=mark):
                piece(way, zb, k, mark).start()

            piece(2, zb, k, s).start()

    def share_moments(which, field):
        mean = jnp.sum(field, axis=0, keepdims=True) * (1.0 / rows)
        offset = field - mean
        square = jnp.sum(offset * offset, axis=0, keepdims=True)
        (near,) = exact_dot([mean], ones[...])
        away = mean - near * (1.0 / size)
        sums, squares = exact_dot([mean, square + rows * (away * away)], fold[...])
        moments[which, r, 0:1, :] = sums * (1.0 / size)
        moments[which, r, 1:2, :] = squares

        for j in sorted(range(1, n), key=lambda j: abs(j - n // 2)):
            stat_copy(which, j).start()

    def gather_moments(which):
        stat_all(which).wait_recv()
        every = moments[which]
        means = every[:, 0, :]
        squares = every[:, 1, :]
        centre = jnp.sum(means, axis=0, keepdims=True) * (1.0 / n)
        away = means - centre
        whole = jnp.sum(squares + (rows * size) * (away * away), axis=0, keepdims=True)
        scale = lax.rsqrt(whole * (1.0 / (n * size * rows)) + EPS)
        return exact_dot([centre, scale], spread[...])

    pl.semaphore_wait(barrier, 3)
    filled(kv.at[z, :, c], load_sem)
    for k in range(chunks):
        if k < early:
            send_own(k)
    def groups(shape, left, right):
        rows_of, columns_of = (lax.broadcasted_iota(jnp.int32, shape, i) for i in (0, 1))
        return jnp.where(rows_of // left == columns_of // right, 1.0, 0.0).astype(jnp.bfloat16)

    def prepare(j):
        if j == 0:
            ones[...] = groups(ones.shape, size, size)
        if j == 1:
            fold[...] = groups(fold.shape, size, 1)
            spread[...] = groups(spread.shape, 1, size)
            maxima[...] = jnp.full_like(maxima, -1e30)
            total[...] = jnp.zeros_like(total)
        if j == 2:
            acc[...] = jnp.zeros_like(acc)

    for j in range(far - 1):
        for target in (upward, downward):
            pl.semaphore_signal(
                entered.at[j], inc=1, device_id=(img, target), device_id_type=MESH
            )
        prepare(j)
        pl.semaphore_wait(entered.at[j], 2)
    pl.semaphore_signal(entered.at[far - 1], inc=1, device_id=(img, partner), device_id_type=MESH)
    pl.semaphore_wait(entered.at[far - 1], 1)
    share_moments(0, own().reshape(rows, channels).astype(jnp.float32))
    for k in range(early, chunks):
        send_own(k)

    for s in range(own_steps, own_steps + primed):
        relay(s)

    filled(mats.at[pl.ds(0, 2)], weight_sem.at[0])
    filled(vectors, vector_sem)
    attn_gain, attn_shift, conv_gain, conv_shift = (vectors[i] for i in range(4))
    conv_bias = vectors[4]
    centre, scale = gather_moments(0)
    gain = scale * attn_gain
    positions = own().reshape(rows, channels).astype(jnp.float32)
    normed = ((positions - centre) * gain + attn_shift).astype(jnp.bfloat16)
    query = jnp.dot(normed, mats[0], preferred_element_type=jnp.float32).astype(jnp.bfloat16)
    folded = lax.dot_general(query, mats[1], NT, preferred_element_type=jnp.float32) * (
        LOG2E / math.sqrt(channels)
    )
    queries[...] = (folded * gain).astype(jnp.bfloat16)
    constant = jnp.sum(folded * (attn_shift - centre * gain), axis=1, keepdims=True)
    bias[...] = jnp.broadcast_to(constant, bias.shape)

    filled(mats.at[pl.ds(2, 2)], weight_sem.at[1])
    wvo[...] = jnp.dot(mats[2], mats[3], preferred_element_type=jnp.float32).astype(jnp.bfloat16)

    filled(wc, weight_sem.at[2])

    @pl.loop(0, 3)
    def _(dx):
        part = pl.ds(pl.multiple_of(dx * channels, channels), channels)
        outer = wc[0, part].astype(jnp.float32) + wc[2, part].astype(jnp.float32)
        inner = wc[1, part].astype(jnp.float32)
        mixed[0, part] = (0.5 * (outer + inner)).astype(jnp.bfloat16)
        mixed[1, part] = (0.5 * (outer - inner)).astype(jnp.bfloat16)

    lanes = 128
    halves = [slice(i, i + rows // 2) for i in range(0, rows, rows // 2)]

    def attend(blocks):
        scores = [
            [
                lax.dot_general(queries[part], block, NT, preferred_element_type=jnp.float32)
                for block in blocks
            ]
            for part in halves
        ]
        for part, pair in zip(halves, scores):
            columns = [
                score[:, j : j + lanes] for score in pair for j in range(0, 2 * chunk, lanes)
            ]
            peak = functools.reduce(jnp.maximum, columns)
            offset = bias[part]
            newest = jnp.maximum(maxima[part], jnp.max(peak, axis=1, keepdims=True) + offset)
            fade = jnp.exp2(maxima[part] - newest)
            maxima[part] = newest
            level = newest - offset
            weights = [jnp.exp2(column - level) for column in columns]
            total[part] = functools.reduce(jnp.add, weights, total[part] * fade)
            each = len(weights) // len(blocks)
            product = 0.0
            for i, block in enumerate(blocks):
                probs = jnp.concatenate(weights[i * each : (i + 1) * each], axis=1)
                product = product + jnp.dot(
                    probs.astype(jnp.bfloat16), block, preferred_element_type=jnp.float32
                )
            acc[part] = acc[part] * jnp.tile(fade, (1, channels // lanes)) + product

    steps = own_steps + (far - 1) * chunks + half_chunks
    first = own_steps + primed - lead
    taper = first + 3

    @pl.loop(0, steps - 1)
    def _(s):
        @pl.when(jnp.logical_and(s >= first, s < taper))
        def _():
            relay(s + lead)

        @pl.when(s >= taper + lead)
        def _():
            relay(s)

        arrived(1, s)
        blocks = []
        for way in (0, 1):
            d, zb, k = spot(way, s)
            blocks.append(kv[zb, k].reshape(2 * chunk, channels))
        attend(blocks)

    final = [spot(way, steps - 1) for way in (0, 1)]
    relay(steps - 1)
    attend([jnp.concatenate([kv[zb, k, c] for d, zb, k in final], axis=0)])
    arrived(1, steps - 1)
    attend([jnp.concatenate([kv[zb, k, 1 - c] for d, zb, k in final], axis=0)])

    denominator = jnp.sum(total[...], axis=1, keepdims=True)
    average = (acc[...] * (1.0 / denominator) - centre) * gain + attn_shift
    attended = jnp.dot(
        average.astype(jnp.bfloat16), wvo[...], preferred_element_type=jnp.float32
    )
    field = (own().reshape(rows, channels).astype(jnp.float32) + attended).astype(jnp.bfloat16)
    hidden[...] = field
    share_moments(1, field.astype(jnp.float32))

    up = pltpu.make_async_remote_copy(
        src_ref=hidden.at[pl.ds(0, wide)],
        dst_ref=halo.at[1],
        send_sem=halo_send.at[1],
        recv_sem=halo_recv.at[1],
        device_id=(img, lax.rem(r + n - 1, n)),
        device_id_type=MESH,
    )
    down = pltpu.make_async_remote_copy(
        src_ref=hidden.at[pl.ds(rows - wide, wide)],
        dst_ref=halo.at[0],
        send_sem=halo_send.at[0],
        recv_sem=halo_recv.at[0],
        device_id=(img, lax.rem(r + 1, n)),
        device_id_type=MESH,
    )

    @pl.when(r > 0)
    def _():
        up.start()

    @pl.when(r < n - 1)
    def _():
        down.start()

    along = kv.at[pl.ds(0, (steps - own_steps) // 2), pl.ds(0, 1)]
    across = kv.at[pl.ds(0, deep // 2)]
    for way, view in enumerate((along, along, across)):
        whole(view, send_sem.at[way], recv_sem.at[0, 0]).wait_send()

    centre, scale = gather_moments(1)
    gain = scale * conv_gain

    def activate(values):
        v = (values.astype(jnp.float32) - centre) * gain + conv_shift
        return (v / (1.0 + jnp.exp(-v))).astype(jnp.bfloat16).astype(jnp.float32)

    column = lax.broadcasted_iota(jnp.int32, (wide, channels), 0)

    def place(term, pair, values):
        at = slice(pair * wide, (pair + 1) * wide)
        before = jnp.where(column > 0, pltpu.roll(values, 1, 0), 0.0)
        after = jnp.where(column < wide - 1, pltpu.roll(values, wide - 1, 0), 0.0)
        for dx, part in enumerate((before, values, after)):
            stacked[term, at, dx * channels : (dx + 1) * channels] = part.astype(jnp.bfloat16)

    def product(term, matrix):
        return jnp.dot(stacked[term], matrix, preferred_element_type=jnp.float32)

    first, second, third, fourth = (
        activate(hidden[y * wide : (y + 1) * wide]) for y in range(lines)
    )
    edge[0] = second
    edge[1] = third
    for pair, (upper, lower) in enumerate(((first, second), (third, fourth))):
        place(1, pair, upper + lower)
        place(2, pair, lower - upper)
    place(0, 1, second - fourth)
    place(3, 0, first - third)
    sums, gaps = product(1, mixed[0]), product(2, mixed[1])
    acc[: rows // 2] = sums + gaps
    acc[rows // 2 :] = sums - gaps

    @pl.when(r > 0)
    def _():
        up.wait_send()
        down.wait_recv()
        edge[2] = activate(halo[0])

    @pl.when(r == 0)
    def _():
        edge[2] = jnp.zeros((wide, channels), jnp.float32)

    @pl.when(r < n - 1)
    def _():
        down.wait_send()
        up.wait_recv()
        edge[3] = activate(halo[1])

    @pl.when(r == n - 1)
    def _():
        edge[3] = jnp.zeros((wide, channels), jnp.float32)

    place(0, 0, edge[2] - edge[0])
    place(3, 1, edge[1] - edge[3])
    evens = acc[: rows // 2] + product(0, wc[0])
    odds = acc[rows // 2 :] - product(3, wc[2])
    for parity, values in enumerate((evens, odds)):
        for pair in range(2):
            y = 2 * pair + parity
            line = slice(y * wide, (y + 1) * wide)
            part = values[pair * wide : (pair + 1) * wide] + conv_bias
            out[line] = (hidden[line].astype(jnp.float32) + part).astype(jnp.bfloat16)

    for which in range(2):
        stat_all(which).wait_send()


def local(n, latent, attn_gain, attn_shift, w_query, w_key, w_value, w_out,
          conv_gain, conv_shift, w_conv, conv_bias):
    height, wide, channels = latent.shape
    rows = height * wide
    chunks = rows // CHUNK
    anywhere = pl.BlockSpec(memory_space=pl.ANY)
    bf16, f32 = jnp.bfloat16, jnp.float32
    square = pltpu.VMEM((channels, channels), bf16)
    dma = pltpu.SemaphoreType.DMA
    def kept(value):
        return pltpu.with_memory_space_constraint(value, pltpu.HBM)

    encoded = pl.pallas_call(
        functools.partial(kernel, n, wide),
        out_shape=jax.ShapeDtypeStruct((rows, channels), bf16),
        in_specs=[anywhere] * 11,
        out_specs=pl.BlockSpec(memory_space=pltpu.VMEM),
        scratch_shapes=[
            pltpu.VMEM((n // 2, chunks, 2, CHUNK, channels), bf16),
            pltpu.VMEM((4, channels, channels), bf16),
            square,
            pltpu.VMEM((3, 3 * channels, channels), bf16),
            square,
            pltpu.VMEM((channels, 128), bf16),
            pltpu.VMEM((128, channels), bf16),
            pltpu.VMEM((2, n, 2, 128), f32),
            pltpu.VMEM((rows, channels), bf16),
            pltpu.VMEM((rows, 128), f32),
            pltpu.VMEM((rows, 128), f32),
            pltpu.VMEM((rows, 128), f32),
            pltpu.VMEM((rows, channels), f32),
            pltpu.VMEM((rows, channels), bf16),
            pltpu.VMEM((2, wide, channels), bf16),
            pltpu.VMEM((4, rows // 2, 3 * channels), bf16),
            dma,
            dma((3,)),
            dma((3,)),
            dma((2, n)),
            dma((2,)),
            dma((2,)),
            dma((2,)),
            dma((2,)),
            pltpu.VMEM((5, 1, channels), f32),
            dma,
            pltpu.SemaphoreType.REGULAR((n // 4,)),
            pltpu.VMEM((2, 3 * channels, channels), bf16),
            pltpu.VMEM((4, wide, channels), f32),
        ],
        compiler_params=pltpu.CompilerParams(
            collective_id=0, has_side_effects=True, vmem_limit_bytes=48 * 1024 * 1024
        ),
    )(
        *map(kept, (latent.reshape(chunks, CHUNK, channels), w_query, w_key, w_value, w_out, w_conv)),
        *(kept(v.reshape(1, channels)) for v in (attn_gain, attn_shift, conv_gain, conv_shift, conv_bias)),
    )
    return encoded.reshape(height, wide, channels)


def solution(mesh):
    in_specs = (P(("img", "row"), None, None), P(), P(), P(), P(), P(), P(), P(), P(), P(), P())
    out_specs = P(("img", "row"), None, None)
    body = functools.partial(local, mesh.shape["row"])
    return jax.shard_map(body, mesh=mesh, in_specs=in_specs, out_specs=out_specs, check_vma=False)
```
